256 devices in a mesh: atom: 16 (over z, core), wave: 16 (over y, x).
Axes of the slice: x: 4, y: 4, z: 8, core: 2. Of those that a mesh axis runs over, the one named last changes fastest.
Arguments:
- features: bfloat16 [131072, 128], P(('atom', 'wave')), may hold values from -6 to 6
- species: int32 [131072], P(('atom', 'wave')), may hold values from 0 to 15
- coords: float32 [3, 131072], P(None, ('atom', 'wave')), may hold values from 0 to 1
- wave_index: int32 [3, 16384], P(None, 'wave'), may hold values from -16 to 16, as said below
- green: float32 [16384], P('wave'), may hold values from 8.631675e-06 to 8.6316744e-05
- embed: bfloat16 [16, 128], replicated, may hold values from -3 to 3
- w_charge: bfloat16 [128, 64], replicated, may hold values from -0.5 to 0.5
- w_feat: bfloat16 [128, 256], replicated, may hold values from -0.5 to 0.5
- w_pot: bfloat16 [64, 256], replicated, may hold values from -0.75 to 0.75
- w_out: bfloat16 [256, 128], replicated, may hold values from -0.375 to 0.375
Outputs:
- updated: bfloat16 [131072, 128], P(('atom', 'wave'))
The draws below stay inside these ranges and needn't reach their ends.
Inputs may be any that keep to these rules, and one draw needn't show every extreme that they name: `wave_index`: the 16384 wave vectors are distinct lattice vectors, and none is zero.
All inputs are finite; a program needn't handle non-finite values.
Results may differ from the reference program's by a relative error of at most 0.0075.
Values may be sent and summed in bfloat16 or wider, within the bound.
A program may use at most 128 MiB of HBM per device.

```python
import math
import jax
import jax.numpy as jnp
from jax import lax

F = 128
Q = 64
HID = 256
SPECIES = 16
NATOMS = 131072
KWAVES = 16384


def draw_wave_index(key, part):
    order = jax.random.permutation(jax.random.fold_in(key, 71), 35936)
    points = order[:KWAVES].astype(jnp.int32)
    points = points + (points >= 17968).astype(jnp.int32)
    first = points // 1089 - 16
    second = points // 33 % 33 - 16
    third = points % 33 - 16
    return jnp.stack([first, second, third]).astype(jnp.int32)


def touch_ends(result, key, smallest, top_value):
    shape = result.shape
    spot = [jax.random.randint(jax.random.fold_in(key, axis), (), 0, shape[axis]) for axis in range(len(shape))]
    result = result.at[tuple(spot)].set(smallest)
    longest = shape.index(max(shape))
    spot[longest] = (spot[longest] + 1) % shape[longest]
    return result.at[tuple(spot)].set(top_value)


def shard_levels(rng, dims, cuts, least, largest):
    factor_of = 1.0
    for position, blocks in cuts:
        heights = jax.random.uniform(jax.random.fold_in(jax.random.fold_in(rng, 6), position), (blocks,), jnp.float32, least / len(cuts), largest / len(cuts))
        factor_of = factor_of * jnp.repeat(jnp.exp(heights), dims[position] // blocks).reshape((-1,) + (1,) * (len(dims) - 1 - position))
    return factor_of


def normal_values(stream_key, shape, spread, bound, cuts=(), kind=jnp.bfloat16):
    result = jax.random.normal(stream_key, shape, jnp.float32) * spread
    if len(cuts) > 0:
        result = shard_levels(stream_key, shape, cuts, -0.22, 0.18) * result
    return jnp.clip(result, min=-bound, max=bound).astype(kind)


def setup_inputs(seed: int = 0) -> dict:
    key_of = jax.random.split(jax.random.key(seed), 11)
    return {
        "features": normal_values(key_of[0], (NATOMS, F), 1.0, 6.0, ((0, 256),)),
        "species": touch_ends(jax.random.randint(key_of[1], (NATOMS,), 0, SPECIES), jax.random.fold_in(key_of[1], 1), 0, SPECIES - 1).astype(jnp.int32),
        "coords": jnp.clip(1.0 * jax.random.uniform(key_of[2], (3, NATOMS), jnp.float32) ** shard_levels(key_of[2], (3, NATOMS), ((1, 256),), -0.2, 0.2), 0.0, 1.0),
        "wave_index": draw_wave_index(jax.random.fold_in(key_of[10], 71), 0),
        "green": jnp.clip(jnp.exp(math.log(8.63167442730628e-05) - 2.30258503 * jax.random.uniform(key_of[4], (KWAVES,), jnp.float32) ** shard_levels(key_of[4], (KWAVES,), ((0, 16),), -0.2, 0.2)), 8.6316749730031e-06, 8.63167442730628e-05),
        "embed": normal_values(key_of[5], (SPECIES, F), 0.5, 3.0),
        "w_charge": normal_values(key_of[6], (F, Q), F ** -0.5, 0.5),
        "w_feat": normal_values(key_of[7], (F, HID), F ** -0.5, 0.5),
        "w_pot": normal_values(key_of[8], (Q, HID), Q ** -0.5, 0.75),
        "w_out": normal_values(key_of[9], (HID, F), HID ** -0.5, 0.375),
    }


TWO_PI = 2.0 * math.pi
EPS = 1e-06

def phases(points, waves):
    angle = points[0][:, None] * waves[0][None, :] + points[1][:, None] * waves[1][None, :]
    angle = TWO_PI * (angle + points[2][:, None] * waves[2][None, :])
    return jnp.concatenate([jnp.cos(angle), jnp.sin(angle)], axis=1).astype(jnp.bfloat16)

def reference(features, species, coords, wave_index, green, embed, w_charge, w_feat, w_pot, w_out):
    hidden_in = features.astype(jnp.float32)
    scale = lax.rsqrt(lax.optimization_barrier(jnp.mean(hidden_in * hidden_in, axis=1, keepdims=True)) + EPS)
    onehot = (species[:, None] == jnp.arange(SPECIES, dtype=jnp.int32)[None, :]).astype(jnp.bfloat16)
    mixed = hidden_in * scale + jnp.dot(onehot, embed, preferred_element_type=jnp.float32)
    mixed_b = mixed.astype(jnp.bfloat16)
    charges = jnp.dot(mixed_b, w_charge, preferred_element_type=jnp.float32).astype(jnp.bfloat16)
    waves = wave_index.astype(jnp.float32)
    step = math.gcd(NATOMS, 2048)
    count = NATOMS // step
    point_blocks = coords.reshape(3, count, step).transpose(1, 0, 2)
    charge_blocks = charges.reshape(count, step, Q)

    def add_block(total, item):
        points, block_charges = item
        tile = phases(points, waves)
        part = lax.dot_general(tile, block_charges, (((0,), (0,)), ((), ())), preferred_element_type=jnp.float32)
        return (total + part, None)
    start = jnp.zeros((2 * KWAVES, Q), jnp.float32)
    structure, _ = lax.scan(add_block, start, (point_blocks, charge_blocks))
    green_both = jnp.concatenate([green, green])
    weighted = (green_both[:, None] * structure).astype(jnp.bfloat16)

    def potential_block(points):
        return jnp.dot(phases(points, waves), weighted, preferred_element_type=jnp.float32)
    potential = lax.map(potential_block, point_blocks).reshape(NATOMS, Q)
    potential_b = potential.astype(jnp.bfloat16)
    pre = jnp.dot(mixed_b, w_feat, preferred_element_type=jnp.float32) + jnp.dot(potential_b, w_pot, preferred_element_type=jnp.float32)
    activation = jax.nn.silu(pre).astype(jnp.bfloat16)
    return (hidden_in + jnp.dot(activation, w_out, preferred_element_type=jnp.float32)).astype(jnp.bfloat16)
```

```python
import functools

import jax
import jax.numpy as jnp
from jax import lax
from jax.experimental import pallas as pl
from jax.experimental.pallas import tpu as pltpu
from jax.sharding import PartitionSpec as P

EPS = 1e-06
N = 16
ATOMS = 512
Q = 64
MAIN = 64 * N
ROWS = MAIN + 9 * N
SHARD = 80
COS = (0.9999999890590228, -19.739204499453827, 64.9391174598908, -85.45013953079768, 60.16763095026347, -25.967599245923736, 6.52865815775625)
SIN = (6.2831853025115025, -41.341700405317205, 81.60513138578321, -76.70301535364746, 42.02592698447418, -14.8998466635365, 3.2381375046186873)
F32 = jnp.float32
BF16 = jnp.bfloat16
NT = (((1,), (1,)), ((), ()))
TN = (((0,), (0,)), ((), ()))


def dot(a, b, dims=(((1,), (0,)), ((), ()))):
    return lax.dot_general(a, b, dims, preferred_element_type=F32)


def poly(u, coeffs):
    total = jnp.full_like(u, coeffs[-1])
    for c in coeffs[-2::-1]:
        total = total * u + c
    return total


def waves_of(x):
    j = lax.broadcasted_iota(jnp.int32, (N, x.shape[1]), 0).astype(F32) + 1.0
    turns = j * x
    r = turns - jnp.round(turns)
    u = r * r
    return poly(u, COS), r * poly(u, SIN)


def green_rows(n1, n2, n3, g, atom, key=None):
    count = n1.shape[1]
    first = jnp.where(n1 != 0, n1, jnp.where(n2 != 0, n2, n3))
    s = jnp.where(first < 0, -1, 1)
    a1, a2, a3 = jnp.abs(n1), jnp.abs(n2), jnp.abs(n3)
    s2 = jnp.where(n2 * s < 0, -1.0, 1.0)
    s3 = jnp.where(n3 * s < 0, -1.0, 1.0)
    row = lax.broadcasted_iota(jnp.int32, (8 * N, count), 0)
    owner, kind = lax.div(row, 8) + 1, lax.rem(row, 8)
    factor = jnp.where((kind == 1) | (kind == 5), s2, 1.0)
    factor = jnp.where(kind == 2, s3, factor)
    factor = jnp.where(kind == 3, s2 * s3, factor)
    inside = a3 == owner
    flat = (a3 == 0) & (a1 == owner)
    line = (a3 == 0) & (n1 == 0) & (a2 == owner)
    hit = jnp.where(kind < 4, inside.astype(F32), jnp.where(kind < 6, flat.astype(F32), line.astype(F32)))
    hit = jnp.where(kind == 7, 0.0, hit)
    left = hit * factor * g
    lane = lax.broadcasted_iota(jnp.int32, (32, count), 0)
    mine = atom + 1
    one, zero = jnp.ones((1, count), F32), jnp.zeros((1, count), F32)
    is1, is2 = (a1 == mine).astype(F32), (a2 == mine).astype(F32)
    no1, no2 = (n1 == 0).astype(F32), (n2 == 0).astype(F32)
    right = jnp.where(lane < N, is1 * (a2 == lane + 1).astype(F32), zero)
    right = jnp.where((lane >= 16) & (lane < 18), is1 * no2, right)
    right = jnp.where((lane >= 18) & (lane < 20), no1 * is2, right)
    right = jnp.where((lane >= 20) & (lane < 24), is2, right)
    right = jnp.where(lane == 24, no1 * no2, right)
    right = jnp.where((lane >= 25) & (lane < 27), no2, right)
    right = jnp.where((lane >= 27) & (lane < 29), one, right)
    right = jnp.concatenate([right, jnp.zeros((96, count), F32)]).astype(BF16)
    total = None
    for _ in range(3):
        piece = left.astype(BF16)
        left = left - piece.astype(F32)
        part = dot(piece, right, NT)
        total = part if total is None else total + part
    return total


def apply_green(t, gt):
    lanes = lax.broadcasted_iota(jnp.int32, (N, 128), 1)
    sign = jnp.where(lanes < Q, -1.0, 1.0)

    def swap(v):
        return jnp.concatenate([v[:, Q:], v[:, :Q]], axis=1)

    cc, cs, sc, ss = t[0:16], t[16:32], t[32:48], t[48:64]
    g0, g2, g3, g23 = (gt[0:16, k : k + 1] for k in range(4))
    xcc, xcs, xsc, xss = sign * swap(cc), sign * swap(cs), sign * swap(sc), sign * swap(ss)
    out = [
        g0 * cc - g2 * ss + g3 * xsc + g23 * xcs,
        g0 * cs + g2 * sc - g23 * xcc + g3 * xss,
        g0 * sc + g2 * cs - g3 * xcc + g23 * xss,
        g0 * ss - g2 * cc - g23 * xsc - g3 * xcs,
    ]
    e = t[64:80]
    r = lax.broadcasted_iota(jnp.int32, (N, 128), 0)
    h = [jnp.broadcast_to(gt[16:32, k : k + 1], (N, 128)) for k in range(8)]
    even = lax.rem(r, 2) == 0
    e0 = jnp.where(r < 4, h[0], jnp.where(r < 8, h[4], jnp.where(r == 8, h[0], jnp.where(r < 11, h[4], h[6]))))
    e0 = jnp.where(r < 13, e0, 0.0)
    e3 = jnp.where(r < 4, jnp.where(even, h[2], -h[2]), 0.0)
    e2 = jnp.where((r >= 4) & (r < 8), jnp.where(r < 6, -h[5], h[5]), 0.0)
    up = jnp.concatenate([e[1:], e[:1]], axis=0)
    down = jnp.concatenate([e[-1:], e[:-1]], axis=0)
    pair = jnp.where(even, up, down)
    out.append(e0 * e + e3 * (sign * swap(pair)) + e2 * pair)
    return jnp.concatenate(out, axis=0)


def kernel(
    feat, species, coords, widx, green, embed, w_charge, w_feat, w_pot, w_out, out,
    cbuf, xbuf, gbuf, gsend, ebuf, zbuf, tabs, tmain, tedge, tsend, trecv, wall, wmain, wedge, wt,
    psend, precv, mixed, pre,
    cs_sem, cr_sem, xs_sem, xr_sem, gs_sem, gr_sem, ts_sem, tr_sem, ws_sem, wr_sem, ps_sem, pr_sem,
):
    atom, wave = lax.axis_index("atom"), lax.axis_index("wave")

    def wave_peer(d):
        y = lax.rem(lax.div(wave, 4) + lax.div(d, 4), 4)
        x = lax.rem(lax.rem(wave, 4) + lax.rem(d, 4), 4)
        return y * 4 + x

    def wave_source(d):
        y = lax.rem(lax.div(wave, 4) + 4 - lax.div(d, 4), 4)
        x = lax.rem(lax.rem(wave, 4) + 4 - lax.rem(d, 4), 4)
        return y * 4 + x

    def atom_peer(d):
        z = lax.rem(lax.div(atom, 2) + lax.div(d, 2), 8)
        return z * 2 + lax.rem(lax.rem(atom, 2) + lax.rem(d, 2), 2)

    def atom_source(d):
        z = lax.rem(lax.div(atom, 2) + 8 - lax.div(d, 2), 8)
        return z * 2 + lax.rem(lax.rem(atom, 2) + lax.rem(d, 2), 2)

    def push(src, dst, ssem, rsem, axis, peer):
        return pltpu.make_async_remote_copy(
            src_ref=src, dst_ref=dst, send_sem=ssem, recv_sem=rsem,
            device_id={axis: peer}, device_id_type=pl.DeviceIdType.MESH,
        )

    def each(body):
        def step(d, carry):
            body(d)
            return carry

        lax.fori_loop(1, N, step, 0)

    barrier = pltpu.get_barrier_semaphore()

    @each
    def _(d):
        pl.semaphore_signal(barrier, inc=1, device_id={"wave": wave_peer(d)}, device_id_type=pl.DeviceIdType.MESH)
        pl.semaphore_signal(barrier, inc=1, device_id={"atom": atom_peer(d)}, device_id_type=pl.DeviceIdType.MESH)

    hidden = feat[...].astype(F32)
    scale = lax.rsqrt(jnp.mean(hidden * hidden, axis=1, keepdims=True) + EPS)
    kinds = lax.broadcasted_iota(jnp.int32, (16, ATOMS), 0)
    onehot = (kinds == species[...]).astype(F32).astype(BF16)
    mixed_b = (hidden * scale + dot(onehot, embed[...], TN)).astype(BF16)
    mixed[...] = mixed_b
    charges = dot(mixed_b, w_charge[...])
    cbuf[wave] = charges.T.astype(BF16)
    xbuf[wave] = coords[...]

    pl.semaphore_wait(barrier, 2 * (N - 1))

    def c_copy(d, slot):
        return push(cbuf.at[slot], cbuf.at[slot], cs_sem.at[d], cr_sem.at[slot], "wave", wave_peer(d))

    def x_copy(d, slot):
        return push(xbuf.at[slot], xbuf.at[slot], xs_sem.at[d], xr_sem.at[slot], "wave", wave_peer(d))

    @each
    def _(d):
        x_copy(d, wave).start()
        c_copy(d, wave).start()

    grid = green_rows(widx[0:1], widx[1:2], widx[2:3], green[...], atom)
    for k in range(N):
        gsend[k] = grid[8 * k : 8 * k + 8]
    gbuf[wave] = gsend[wave]

    def g_copy(d, slot):
        return push(gsend.at[wave_peer(d)], gbuf.at[slot], gs_sem.at[d], gr_sem.at[slot], "wave", wave_peer(d))

    @each
    def _(d):
        g_copy(d, wave).start()

    tmain[...] = jnp.zeros_like(tmain)
    tedge[...] = jnp.zeros_like(tedge)

    def add_block(slot):
        place = xbuf[slot]
        xc, xs = waves_of(place[0:1])
        yc, ys = waves_of(place[1:2])
        zc, zs = waves_of(place[2:3])
        for k, table in enumerate((xc, xs, yc, ys, zc, zs)):
            tabs[k] = table
        xcw, xsw, ycw, ysw, zcw, zsw = (tabs[k, pl.ds(wave, 1), :] for k in range(6))
        for i in range(N):
            a, b = xc[i : i + 1], xs[i : i + 1]
            block = jnp.concatenate([a * yc, a * ys, b * yc, b * ys], axis=0)
            ebuf[slot, 64 * i : 64 * i + 64, :] = block.astype(BF16)
        r = lax.broadcasted_iota(jnp.int32, (N, ATOMS), 0)
        rest = jnp.where(r == 0, 1.0, 0.0)
        for k, row in enumerate((xcw, xsw, ycw, ysw)):
            rest = jnp.where(r == k + 1, row, rest)
        edge = (xc, xs, yc, ys, xcw * yc, xsw * ys, xsw * yc, xcw * ys, rest)
        for k, part in enumerate(edge):
            ebuf[slot, MAIN + N * k : MAIN + N * (k + 1), :] = part.astype(BF16)
        zbuf[slot] = jnp.concatenate([zcw, zsw, jnp.zeros((6, ATOMS), F32)], axis=0)
        c = cbuf[slot]
        wide = c.astype(F32)
        cz = jnp.concatenate([zcw * wide, zsw * wide], axis=0).astype(BF16)
        full = jnp.concatenate([cz, c, jnp.zeros((Q, ATOMS), BF16)], axis=0)
        for k in range(4):
            rows = slice(256 * k, 256 * k + 256)
            tmain[rows, :] += dot(ebuf[slot, rows, :], cz, NT)
        tedge[...] += dot(ebuf[slot, MAIN:, :], full, NT)

    add_block(wave)

    @each
    def _(d):
        slot = wave_source(d)
        x_copy(d, slot).wait_recv()
        c_copy(d, slot).wait_recv()
        add_block(slot)

    r = lax.broadcasted_iota(jnp.int32, (9 * N, 128), 0)
    flat = ((r >= 4 * N) & (r < 8 * N)) | (r > 8 * N)
    wedge[...] = jnp.where(flat, tedge[:, 128:], tedge[:, :128])
    for i in range(N):
        tsend[i, 0:64, :] = tmain[64 * i : 64 * i + 64, :].astype(BF16)
        tail = jnp.concatenate([wedge[pl.ds(i, 8, stride=N), :], wedge[8 * N : 8 * N + 8, :]], axis=0)
        tsend[i, 64:80, :] = tail.astype(BF16)

    def t_copy(d, slot):
        return push(tsend.at[atom_peer(d)], trecv.at[slot], ts_sem.at[d], tr_sem.at[slot], "atom", atom_peer(d))

    @each
    def _(d):
        t_copy(d, atom).start()

    trecv[atom] = tsend[atom]
    pre[...] = dot(mixed[...], w_feat[...])

    @each
    def _(d):
        g_copy(d, wave_source(d)).wait_recv()

    gsum = gbuf[0]
    for k in range(1, N):
        gsum = gsum + gbuf[k]
    columns = jnp.concatenate([gsum, jnp.zeros((120, 128), F32)], axis=0).T

    @each
    def _(d):
        t_copy(d, atom_source(d)).wait_recv()

    total = trecv[0].astype(F32)
    for k in range(1, N):
        total = total + trecv[k].astype(F32)
    wall[atom] = apply_green(total, columns).astype(BF16)

    def w_copy(d, slot):
        return push(wall.at[slot], wall.at[slot], ws_sem.at[d], wr_sem.at[slot], "atom", atom_peer(d))

    @each
    def _(d):
        w_copy(d, atom).start()

    @each
    def _(d):
        w_copy(d, atom_source(d)).wait_recv()

    for i in range(N):
        shard = wall[i].astype(F32)
        wmain[64 * i : 64 * i + 64, :] = shard[0:64]
        wedge[pl.ds(i, 8, stride=N), :] = shard[64:72]
        if i == 0:
            wedge[8 * N : 9 * N, :] = jnp.concatenate([shard[72:80], jnp.zeros((8, 128), F32)], axis=0)
    for k in range(8):
        wt[0:128, 128 * k : 128 * k + 128] = wmain[128 * k : 128 * k + 128, :].T.astype(BF16)
    wt[128:192, 0:MAIN] = jnp.zeros((64, MAIN), BF16)
    edges = wedge[...]
    low = jnp.where(flat, 0.0, edges)
    high = jnp.where(flat, edges, 0.0)
    blank = jnp.zeros((112, 128), F32)
    low_t = jnp.concatenate([low[:128].T, jnp.concatenate([low[128:], blank], axis=0).T], axis=1)
    high_t = jnp.concatenate([high[:128].T, jnp.concatenate([high[128:], blank], axis=0).T], axis=1)
    wt[0:128, MAIN:] = low_t[:, : 9 * N].astype(BF16)
    wt[128:192, MAIN:] = high_t[:Q, : 9 * N].astype(BF16)

    def p_copy(d, slot):
        return push(psend.at[wave_peer(d)], precv.at[slot], ps_sem.at[d], pr_sem.at[slot], "wave", wave_peer(d))

    def partial(slot):
        u = dot(wt[...], ebuf[slot])
        z = zbuf[slot]
        return (z[0:1] * u[0:Q] + z[1:2] * u[Q : 2 * Q] + u[2 * Q :]).astype(BF16)

    @each
    def _(d):
        slot = wave_peer(d)
        psend[slot] = partial(slot)
        p_copy(d, wave).start()

    precv[wave] = partial(wave)

    @each
    def _(d):
        p_copy(d, wave_source(d)).wait_recv()

    potential = precv[0].astype(F32)
    for k in range(1, N):
        potential = potential + precv[k].astype(F32)
    potential_b = potential.T.astype(BF16)
    before = pre[...] + dot(potential_b, w_pot[...])
    activation = (before / (1.0 + jnp.exp(-before))).astype(BF16)
    out[...] = (feat[...].astype(F32) + dot(activation, w_out[...])).astype(BF16)

    @each
    def _(d):
        x_copy(d, wave).wait_send()
        c_copy(d, wave).wait_send()
        g_copy(d, wave).wait_send()
        t_copy(d, atom).wait_send()
        w_copy(d, atom).wait_send()
        p_copy(d, wave).wait_send()


def shards(features, species, coords, wave_index, green, embed, w_charge, w_feat, w_pot, w_out):
    vmem = pl.BlockSpec(memory_space=pltpu.VMEM)
    dma = pltpu.SemaphoreType.DMA((N,))
    return pl.pallas_call(
        kernel,
        out_shape=jax.ShapeDtypeStruct(features.shape, BF16),
        in_specs=[vmem] * 10,
        out_specs=vmem,
        scratch_shapes=[
            pltpu.VMEM((N, Q, ATOMS), BF16),
            pltpu.VMEM((N, 3, ATOMS), F32),
            pltpu.VMEM((N, 8, 128), F32),
            pltpu.VMEM((N, 8, 128), F32),
            pltpu.VMEM((N, ROWS, ATOMS), BF16),
            pltpu.VMEM((N, 8, ATOMS), F32),
            pltpu.VMEM((6, N, ATOMS), F32),
            pltpu.VMEM((MAIN, 128), F32),
            pltpu.VMEM((9 * N, 256), F32),
            pltpu.VMEM((N, SHARD, 128), BF16),
            pltpu.VMEM((N, SHARD, 128), BF16),
            pltpu.VMEM((N, SHARD, 128), BF16),
            pltpu.VMEM((MAIN, 128), F32),
            pltpu.VMEM((9 * N, 128), F32),
            pltpu.VMEM((192, ROWS), BF16),
            pltpu.VMEM((N, Q, ATOMS), BF16),
            pltpu.VMEM((N, Q, ATOMS), BF16),
            pltpu.VMEM((ATOMS, 128), BF16),
            pltpu.VMEM((ATOMS, 256), F32),
        ]
        + [dma] * 12,
        compiler_params=pltpu.CompilerParams(
            collective_id=0, has_side_effects=True, vmem_limit_bytes=60 * 1024 * 1024
        ),
        name="ewald",
    )(
        features, species.reshape(1, -1), coords, wave_index, green.reshape(1, -1),
        embed, w_charge, w_feat, w_pot, w_out,
    )


def solution(mesh):
    placed = (
        P(("atom", "wave"), None),
        P(("atom", "wave")),
        P(None, ("atom", "wave")),
        P(None, "wave"),
        P("wave"),
        P(),
        P(),
        P(),
        P(),
        P(),
    )
    return jax.shard_map(
        shards, mesh=mesh, in_specs=placed, out_specs=P(("atom", "wave"), None), check_vma=False
    )
```

```python
import functools

import jax
import jax.numpy as jnp
from jax import lax
from jax.experimental import pallas as pl
from jax.experimental.pallas import tpu as pltpu
from jax.sharding import PartitionSpec as P

EPS = 1e-06
N = 16
ATOMS = 512
Q = 64
MAIN = 64 * N
LOW = MAIN + 5 * N
ROWS = LOW + 5 * N
SHARD = 80
COS = (0.9999999890590228, -19.739204499453827, 64.9391174598908, -85.45013953079768, 60.16763095026347, -25.967599245923736, 6.52865815775625)
SIN = (6.2831853025115025, -41.341700405317205, 81.60513138578321, -76.70301535364746, 42.02592698447418, -14.8998466635365, 3.2381375046186873)
F32 = jnp.float32
BF16 = jnp.bfloat16
NT = (((1,), (1,)), ((), ()))
TN = (((0,), (0,)), ((), ()))


def dot(a, b, dims=(((1,), (0,)), ((), ()))):
    return lax.dot_general(a, b, dims, preferred_element_type=F32)


def poly(u, coeffs):
    total = jnp.full_like(u, coeffs[-1])
    for c in coeffs[-2::-1]:
        total = total * u + c
    return total


def waves_of(x):
    j = lax.broadcasted_iota(jnp.int32, (8, x.shape[1]), 0).astype(F32) + 1.0
    turns = j * x
    r = turns - jnp.round(turns)
    u = r * r
    c, s = poly(u, COS), r * poly(u, SIN)
    c8, s8 = c[7:8], s[7:8]
    return jnp.concatenate([c, c8 * c - s8 * s], axis=0), jnp.concatenate([s, s8 * c + c8 * s], axis=0)


def green_rows(n1, n2, n3, g, atom, key=None):
    count = n1.shape[1]
    first = jnp.where(n1 != 0, n1, jnp.where(n2 != 0, n2, n3))
    s = jnp.where(first < 0, -1, 1)
    a1, a2, a3 = jnp.abs(n1), jnp.abs(n2), jnp.abs(n3)
    s2 = jnp.where(n2 * s < 0, -1.0, 1.0)
    s3 = jnp.where(n3 * s < 0, -1.0, 1.0)
    row = lax.broadcasted_iota(jnp.int32, (8 * N, count), 0)
    owner, kind = lax.div(row, 8) + 1, lax.rem(row, 8)
    factor = jnp.where((kind == 1) | (kind == 5), s2, 1.0)
    factor = jnp.where(kind == 2, s3, factor)
    factor = jnp.where(kind == 3, s2 * s3, factor)
    inside = a3 == owner
    flat = (a3 == 0) & (a1 == owner)
    line = (a3 == 0) & (n1 == 0) & (a2 == owner)
    hit = jnp.where(kind < 4, inside.astype(F32), jnp.where(kind < 6, flat.astype(F32), line.astype(F32)))
    hit = jnp.where(kind == 7, 0.0, hit)
    left = hit * factor * g
    lane = lax.broadcasted_iota(jnp.int32, (32, count), 0)
    mine = atom + 1
    one, zero = jnp.ones((1, count), F32), jnp.zeros((1, count), F32)
    is1, is2 = (a1 == mine).astype(F32), (a2 == mine).astype(F32)
    no1, no2 = (n1 == 0).astype(F32), (n2 == 0).astype(F32)
    right = jnp.where(lane < N, is1 * (a2 == lane + 1).astype(F32), zero)
    right = jnp.where((lane >= 16) & (lane < 18), is1 * no2, right)
    right = jnp.where((lane >= 18) & (lane < 20), no1 * is2, right)
    right = jnp.where((lane >= 20) & (lane < 24), is2, right)
    right = jnp.where(lane == 24, no1 * no2, right)
    right = jnp.where((lane >= 25) & (lane < 27), no2, right)
    right = jnp.where((lane >= 27) & (lane < 29), one, right)
    right = jnp.concatenate([right, jnp.zeros((96, count), F32)]).astype(BF16)
    total = None
    for _ in range(3):
        piece = left.astype(BF16)
        left = left - piece.astype(F32)
        part = dot(piece, right, NT)
        total = part if total is None else total + part
    return total


def apply_green(t, gt):
    lanes = lax.broadcasted_iota(jnp.int32, (N, 128), 1)
    sign = jnp.where(lanes < Q, -1.0, 1.0)

    def swap(v):
        return jnp.concatenate([v[:, Q:], v[:, :Q]], axis=1)

    cc, cs, sc, ss = t[0:16], t[16:32], t[32:48], t[48:64]
    g0, g2, g3, g23 = (gt[0:16, k : k + 1] for k in range(4))
    xcc, xcs, xsc, xss = sign * swap(cc), sign * swap(cs), sign * swap(sc), sign * swap(ss)
    out = [
        g0 * cc - g2 * ss + g3 * xsc + g23 * xcs,
        g0 * cs + g2 * sc - g23 * xcc + g3 * xss,
        g0 * sc + g2 * cs - g3 * xcc + g23 * xss,
        g0 * ss - g2 * cc - g23 * xsc - g3 * xcs,
    ]
    e = t[64:80]
    r = lax.broadcasted_iota(jnp.int32, (N, 128), 0)
    h = [jnp.broadcast_to(gt[16:32, k : k + 1], (N, 128)) for k in range(8)]
    even = lax.rem(r, 2) == 0
    e0 = jnp.where(r < 4, h[0], jnp.where(r < 8, h[4], jnp.where(r == 8, h[0], jnp.where(r < 11, h[4], h[6]))))
    e0 = jnp.where(r < 13, e0, 0.0)
    e3 = jnp.where(r < 4, jnp.where(even, h[2], -h[2]), 0.0)
    e2 = jnp.where((r >= 4) & (r < 8), jnp.where(r < 6, -h[5], h[5]), 0.0)
    up = jnp.concatenate([e[1:], e[:1]], axis=0)
    down = jnp.concatenate([e[-1:], e[:-1]], axis=0)
    pair = jnp.where(even, up, down)
    out.append(e0 * e + e3 * (sign * swap(pair)) + e2 * pair)
    return jnp.concatenate(out, axis=0)


def pick(k, values):
    out = values[-1]
    for j in range(len(values) - 2, -1, -1):
        out = jnp.where(k == j, values[j], out)
    return out


def kernel(
    feat_in, species_in, coords_in, widx_in, green_in, embed_in, wc_in, wf_in, wp_in, wo_in, out,
    feat, species, coords, widx, green, embed, w_charge_t, w_feat, w_pot, w_out,
    cbuf, xbuf, gbuf, gsend, ebuf, zbuf, tabs, tabs_too, czs, tmain, tedge, wedge, thalf, tother, tsend, trecv, wall, wt,
    psend, precv, prelay, mixed, pre,
    in_sem, send_sem, cr_sem, xr_sem, gr_sem, th_sem, tr_sem, wr_sem, pr_sem, pq_sem,
):
    atom, wave = lax.axis_index("atom"), lax.axis_index("wave")
    here_y, here_x = lax.div(wave, 4), lax.rem(wave, 4)
    z, core = lax.div(atom, 2), lax.rem(atom, 2)
    partner = 2 * z + 1 - core
    ahead = 1 + 2 * core
    back = 3 - 2 * core

    def at(dy, dx):
        return lax.rem(here_y + dy, 4) * 4 + lax.rem(here_x + dx, 4)

    def opposite(dy, dx):
        return at(4 - dy, 4 - dx)

    PLACE_Y = (3, 1, 1, 3, 0, ahead, 0, back, 2, 1, 2, 3, 0, 2, 2)
    PLACE_X = (1, 1, 3, 3, ahead, 0, back, 0, 1, 2, 3, 2, 2, 0, 2)
    STEP_Y = (3, 0, 1, 0, 0, ahead, ahead)
    STEP_X = (0, 1, 0, 3, ahead, 0, ahead)
    corner = 1 + 2 * core

    def z_atom(dz, side):
        return 2 * lax.rem(z + dz, 8) + side

    def push(src, dst, ssem, rsem, axis, peer):
        return pltpu.make_async_remote_copy(
            src_ref=src, dst_ref=dst, send_sem=ssem, recv_sem=rsem,
            device_id={axis: peer}, device_id_type=pl.DeviceIdType.MESH,
        )

    def times(count, body, start=0):
        def step(k, carry):
            body(k)
            return carry

        lax.fori_loop(start, count, step, 0)

    barrier = pltpu.get_barrier_semaphore()

    def greet(axis, peer):
        pl.semaphore_signal(barrier, inc=1, device_id={axis: peer}, device_id_type=pl.DeviceIdType.MESH)

    for d in (4, 3, 5, 2, 6, 1, 7):
        greet("atom", z_atom(d, core))
    times(N, lambda d: greet("wave", at(lax.div(d, 4), lax.rem(d, 4))), 1)
    greet("atom", partner)

    loads = [
        pltpu.make_async_copy(src, dst, in_sem.at[k])
        for k, (src, dst) in enumerate(
            (
                (feat_in, feat), (species_in, species), (coords_in, coords), (embed_in, embed), (wc_in, w_charge_t),
                (widx_in, widx), (green_in, green), (wf_in, w_feat), (wp_in, w_pot), (wo_in, w_out),
            )
        )
    ]
    for load in loads:
        load.start()
    for load in loads[:5]:
        load.wait()

    hidden = feat[...].astype(F32)
    scale = lax.rsqrt(jnp.mean(hidden * hidden, axis=1, keepdims=True) + EPS)
    kinds = lax.broadcasted_iota(jnp.int32, (16, ATOMS), 0)
    onehot = (kinds == species[...]).astype(F32).astype(BF16)
    mixed_b = (hidden * scale + dot(onehot, embed[...], TN)).astype(BF16)
    mixed[...] = mixed_b
    cbuf[wave] = dot(w_charge_t[...], mixed_b, NT).astype(BF16)
    xbuf[wave] = coords[...]

    tmain[...] = jnp.zeros_like(tmain)
    tedge[...] = jnp.zeros_like(tedge)

    def prepare(slot, tabs, czs):
        place = xbuf[slot]
        for k in range(3):
            tabs[2 * k], tabs[2 * k + 1] = waves_of(place[k : k + 1])
        zcw, zsw = (tabs[k, pl.ds(wave, 1), :] for k in (4, 5))
        zbuf[slot] = jnp.concatenate([zcw, zsw, jnp.zeros((6, ATOMS), F32)], axis=0)
        wide = cbuf[slot].astype(F32)
        czs[...] = jnp.concatenate([zcw * wide, zsw * wide], axis=0).T.astype(BF16)

    def multiply(slot, tabs, czs):
        xc, xs, yc, ys = (tabs[k] for k in range(4))
        xcw, xsw, ycw, ysw = (tabs[k, pl.ds(wave, 1), :] for k in range(4))
        for i in range(N):
            a, b = xc[i : i + 1], xs[i : i + 1]
            for k, part in enumerate((a * yc, a * ys, b * yc, b * ys)):
                ebuf[slot, 64 * i + N * k : 64 * i + N * (k + 1), :] = part.astype(BF16)
        r = lax.broadcasted_iota(jnp.int32, (N, ATOMS), 0)
        one = jnp.where(r == 0, 1.0, 0.0)
        rest = jnp.zeros((N, ATOMS), F32)
        for k, row in enumerate((xcw, xsw, ycw, ysw)):
            rest = jnp.where(r == k + 1, row, rest)
        edge = (one, xc, xs, yc, ys, xcw * yc, xsw * ys, xsw * yc, xcw * ys, rest)
        for k, part in enumerate(edge):
            ebuf[slot, MAIN + N * k : MAIN + N * (k + 1), :] = part.astype(BF16)
        tmain[...] += dot(ebuf[slot, :LOW, :], czs[...])
        tedge[...] += dot(ebuf[slot, LOW:, :], cbuf[slot], NT)

    pl.semaphore_wait(barrier, 7 + 15 + 1)

    def c_copy(slot, peer):
        return push(cbuf.at[slot], cbuf.at[slot], send_sem.at[0], cr_sem.at[slot], "wave", peer)

    def x_copy(slot, peer):
        return push(xbuf.at[slot], xbuf.at[slot], send_sem.at[1], xr_sem.at[slot], "wave", peer)

    def send_on(slot, peer):
        x_copy(slot, peer).start()
        c_copy(slot, peer).start()

    for k in (1, 3, 0, 2, 4, 5, 6, 7):
        send_on(wave, at(PLACE_Y[k], PLACE_X[k]))

    for load in loads[5:]:
        load.wait()
    grid = green_rows(widx[0:1], widx[1:2], widx[2:3], green[...], atom)
    for k in range(N):
        gsend[k] = grid[8 * k : 8 * k + 8]
    gbuf[0] = gsend[wave]

    @functools.partial(times, N, start=1)
    def _(d):
        peer = at(lax.div(d, 4), lax.rem(d, 4))
        push(gsend.at[peer], gbuf.at[d], send_sem.at[2], gr_sem.at[0], "wave", peer).start()

    prepare(wave, tabs, czs)

    received = []
    for k in (1, 3, 0, 2, 4, 5, 6, 7, 9, 11, 8, 10, 12, 13, 14):
        code = PLACE_Y[k] + 4 * PLACE_X[k]
        if k < 6:
            code = code + 16 * STEP_Y[k] + 64 * STEP_X[k] + 256
        received.append(code)

    def receive(turn):
        code = pick(turn, received)
        slot = opposite(lax.rem(code, 4), lax.rem(lax.div(code, 4), 4))
        x_copy(slot, slot).wait_recv()
        c_copy(slot, slot).wait_recv()

        @pl.when(turn < 6)
        def _():
            send_on(slot, at(lax.rem(lax.div(code, 16), 4), lax.rem(lax.div(code, 64), 4)))

        @pl.when(turn == core)
        def _():
            send_on(slot, at(ahead, ahead))

        return slot

    def one(j, current):
        following = receive(j)
        for k in range(4):
            tabs_too[k] = tabs[k]
        multiply(current, tabs_too, czs)
        prepare(following, tabs, czs)
        return following

    current = lax.fori_loop(0, 15, one, wave)
    multiply(current, tabs, czs)

    wedge[0 : 4 * N, :] = tmain[MAIN + N : LOW, :]
    wedge[4 * N :, :] = jnp.concatenate([tedge[...], jnp.zeros((5 * N, Q), F32)], axis=1)
    wedge[8 * N : 8 * N + 8, :] += tmain[MAIN : MAIN + 8, :]

    def shard(i):
        main = tmain[pl.ds(pl.multiple_of(64 * i, 64), 64), :]
        return jnp.concatenate([main, wedge[pl.ds(i, 8, stride=N), :], wedge[8 * N : 8 * N + 8, :]], axis=0)

    for k in range(8):
        thalf[k] = shard(2 * k + 1 - core).astype(BF16)
    half_copy = push(thalf, tother, th_sem.at[0], th_sem.at[1], "atom", partner)
    half_copy.start()
    pre[...] = dot(mixed[...], w_feat[...])
    push(gsend.at[0:15], gbuf.at[1:16], send_sem.at[2], gr_sem.at[0], "wave", wave).wait_recv()
    gsum = gbuf[0]
    for k in range(1, N):
        gsum = gsum + gbuf[k]
    columns = jnp.concatenate([gsum, jnp.zeros((120, 128), F32)], axis=0).T

    half_copy.wait_recv()

    def t_copy(d):
        return push(tsend.at[d], trecv.at[d], send_sem.at[3], tr_sem.at[0], "atom", z_atom(d, core))

    for d in (4, 3, 5, 2, 6, 1, 7):
        owner = lax.rem(z + d, 8)
        tsend[d] = (shard(2 * owner + core) + tother[owner].astype(F32)).astype(BF16)
        t_copy(d).start()
    total = shard(atom) + tother[z].astype(F32)

    all_shards = push(tsend.at[1:8], trecv.at[1:8], send_sem.at[3], tr_sem.at[0], "atom", atom)
    all_shards.wait_recv()
    for d in range(1, 8):
        total = total + trecv[d].astype(F32)
    wall[atom] = apply_green(total, columns).astype(BF16)

    def w_copy(slot, peer):
        return push(wall.at[slot], wall.at[slot], send_sem.at[4], wr_sem.at[slot], "atom", peer)

    for d in (4, 3, 5, 2, 6, 1, 7):
        w_copy(atom, z_atom(d, core)).start()
    w_copy(atom, partner).start()
    wt[128:192, 0:MAIN] = jnp.zeros((64, MAIN), BF16)

    def place_pair(d):
        ring = lax.rem(z + 8 - d, 8)
        w_copy(2 * ring + 1 - core, partner).wait_recv()
        first, second = wall[2 * ring].astype(F32), wall[2 * ring + 1].astype(F32)
        pair = jnp.concatenate([first[0:64], second[0:64]], axis=0)
        wt[0:128, pl.ds(pl.multiple_of(128 * ring, 128), 128)] = pair.T.astype(BF16)
        wedge[pl.ds(2 * ring, 8, stride=N), :] = first[64:72]
        wedge[pl.ds(2 * ring + 1, 8, stride=N), :] = second[64:72]

    order = (0, 1, 7, 2, 6, 3, 5, 4)
    for j, d in enumerate(order):
        if d:
            source = z_atom(8 - d, core)
            w_copy(source, partner).wait_recv()
            w_copy(source, partner).start()
        if j >= 2:
            place_pair(order[j - 2])
    for d in order[-2:]:
        place_pair(d)
    tail = jnp.concatenate([wall[0, 72:80, :].astype(F32), jnp.zeros((8, 128), F32)], axis=0)
    edges = jnp.concatenate([tail, wedge[0 : 8 * N, :], tail, jnp.zeros((96, 128), F32)], axis=0)
    edges = jnp.concatenate([edges[:128].T, edges[128:].T], axis=1)
    column = lax.broadcasted_iota(jnp.int32, (128, 256), 1)
    low = jnp.where((column == 0) | ((column >= N) & (column < 5 * N)), edges, 0.0)
    high = jnp.where((column >= 5 * N) & (column != 9 * N), edges, 0.0)
    wt[0:128, MAIN:] = low[:, : ROWS - MAIN].astype(BF16)
    wt[128:192, MAIN:] = high[:Q, : ROWS - MAIN].astype(BF16)

    prelay[7] = jnp.zeros((Q, ATOMS), BF16)

    def partial(slot):
        u = dot(wt[...], ebuf[slot])
        v = zbuf[slot]
        return v[0:1] * u[0:Q] + v[1:2] * u[Q : 2 * Q] + u[2 * Q :]

    def up_copy(k, peer):
        return push(psend.at[k], precv.at[k], send_sem.at[5], pr_sem.at[k], "wave", peer)

    def relay_copy(k, r, peer):
        return push(psend.at[k], prelay.at[r], send_sem.at[5], pq_sem.at[r], "wave", peer)

    across = 4 - corner
    turns = (14, 8 + corner, 8, 10, 8 + across, 12, 13, 6, 7, 0, 2, corner, across, 4, 5)

    @functools.partial(times, 15)
    def _(j):
        k = pick(j, turns)
        slot = opposite(pick(k, PLACE_Y), pick(k, PLACE_X))
        value = partial(slot)

        @pl.when(k < 6)
        def _():
            relay_copy(0, k, slot).wait_recv()

        @pl.when(k == corner)
        def _():
            relay_copy(0, 6, slot).wait_recv()

        value = value + prelay[jnp.where(k < 6, k, 7)].astype(F32)
        value = value + prelay[jnp.where(k == corner, 6, 7)].astype(F32)
        psend[k] = value.astype(BF16)

        @pl.when(k < 8)
        def _():
            up_copy(k, slot).start()

        @pl.when(k >= 8)
        def _():
            step = k - 8
            relay_copy(k, step, opposite(pick(step, STEP_Y), pick(step, STEP_X))).start()

    potential = partial(wave)
    for k in (6, 7, 0, 2, 1, 3, 4, 5):
        up_copy(k, wave).wait_recv()
        potential = potential + precv[k].astype(F32)
    potential_b = potential.T.astype(BF16)
    before = pre[...] + dot(potential_b, w_pot[...])
    activation = (before / (1.0 + jnp.exp(-before))).astype(BF16)
    out[...] = (feat[...].astype(F32) + dot(activation, w_out[...])).astype(BF16)

    half_copy.wait_send()
    all_shards.wait_send()
    push(cbuf.at[0:15], cbuf.at[0:15], send_sem.at[0], cr_sem.at[0], "wave", wave).wait_send()
    push(xbuf.at[0:15], xbuf.at[0:15], send_sem.at[1], xr_sem.at[0], "wave", wave).wait_send()
    push(gsend.at[0:15], gbuf.at[1:16], send_sem.at[2], gr_sem.at[0], "wave", wave).wait_send()
    push(wall.at[0:15], wall.at[0:15], send_sem.at[4], wr_sem.at[0], "atom", atom).wait_send()
    push(psend, psend, send_sem.at[5], pr_sem.at[0], "wave", wave).wait_send()


def shards(features, species, coords, wave_index, green, embed, w_charge, w_feat, w_pot, w_out):
    operands = (
        features, species.reshape(1, -1), coords, wave_index, green.reshape(1, -1),
        embed, w_charge.T, w_feat, w_pot, w_out,
    )
    return pl.pallas_call(
        kernel,
        out_shape=pltpu.VMEM(features.shape, BF16),
        in_specs=[pl.BlockSpec(memory_space=pl.ANY)] * 10,
        out_specs=pl.BlockSpec(memory_space=pltpu.VMEM),
        scratch_shapes=[pltpu.VMEM(v.shape, v.dtype) for v in operands]
        + [
            pltpu.VMEM((N, Q, ATOMS), BF16),
            pltpu.VMEM((N, 3, ATOMS), F32),
            pltpu.VMEM((N, 8, 128), F32),
            pltpu.VMEM((N, 8, 128), F32),
            pltpu.VMEM((N, ROWS, ATOMS), BF16),
            pltpu.VMEM((N, 8, ATOMS), F32),
            pltpu.VMEM((6, N, ATOMS), F32),
            pltpu.VMEM((6, N, ATOMS), F32),
            pltpu.VMEM((ATOMS, 128), BF16),
            pltpu.VMEM((LOW, 128), F32),
            pltpu.VMEM((5 * N, Q), F32),
            pltpu.VMEM((9 * N, 128), F32),
            pltpu.VMEM((8, SHARD, 128), BF16),
            pltpu.VMEM((8, SHARD, 128), BF16),
            pltpu.VMEM((8, SHARD, 128), BF16),
            pltpu.VMEM((8, SHARD, 128), BF16),
            pltpu.VMEM((N, SHARD, 128), BF16),
            pltpu.VMEM((192, ROWS), BF16),
            pltpu.VMEM((15, Q, ATOMS), BF16),
            pltpu.VMEM((8, Q, ATOMS), BF16),
            pltpu.VMEM((8, Q, ATOMS), BF16),
            pltpu.VMEM((ATOMS, 128), BF16),
            pltpu.VMEM((ATOMS, 256), F32),
        ]
        + [pltpu.SemaphoreType.DMA((n,)) for n in (10, 6, N, N, 1, 2, 1, N, 8, 7)],
        compiler_params=pltpu.CompilerParams(
            collective_id=0, has_side_effects=True, vmem_limit_bytes=60 * 1024 * 1024
        ),
        name="ewald",
    )(*operands)


def solution(mesh):
    placed = (
        P(("atom", "wave"), None),
        P(("atom", "wave")),
        P(None, ("atom", "wave")),
        P(None, "wave"),
        P("wave"),
        P(),
        P(),
        P(),
        P(),
        P(),
    )
    return jax.shard_map(
        shards, mesh=mesh, in_specs=placed, out_specs=P(("atom", "wave"), None), check_vma=False
    )
```

```python
import functools

import jax
import jax.numpy as jnp
from jax import lax
from jax.experimental import pallas as pl
from jax.experimental.pallas import tpu as pltpu
from jax.sharding import PartitionSpec as P

EPS = 1e-06
N = 16
ATOMS = 512
Q = 64
HALF = N // 2
MAIN = 64 * HALF
LOW = MAIN + 6 * N
ROWS = LOW + 5 * N
SHARD = 80
COS = (0.9999999890590228, -19.739204499453827, 64.9391174598908, -85.45013953079768, 60.16763095026347, -25.967599245923736, 6.52865815775625)
SIN = (6.2831853025115025, -41.341700405317205, 81.60513138578321, -76.70301535364746, 42.02592698447418, -14.8998466635365, 3.2381375046186873)
F32 = jnp.float32
BF16 = jnp.bfloat16
NT = (((1,), (1,)), ((), ()))
TN = (((0,), (0,)), ((), ()))


def dot(a, b, dims=(((1,), (0,)), ((), ()))):
    return lax.dot_general(a, b, dims, preferred_element_type=F32)


def poly(u, coeffs):
    total = jnp.full_like(u, coeffs[-1])
    for c in coeffs[-2::-1]:
        total = total * u + c
    return total


def circle(turns):
    r = turns - jnp.round(turns)
    u = r * r
    return poly(u, COS), r * poly(u, SIN)


def green_rows(n1, n2, n3, g, atom, key=None):
    count = n1.shape[1]
    first = jnp.where(n1 != 0, n1, jnp.where(n2 != 0, n2, n3))
    s = jnp.where(first < 0, -1, 1)
    a1, a2, a3 = jnp.abs(n1), jnp.abs(n2), jnp.abs(n3)
    s2 = jnp.where(n2 * s < 0, -1.0, 1.0)
    s3 = jnp.where(n3 * s < 0, -1.0, 1.0)
    row = lax.broadcasted_iota(jnp.int32, (8 * N, count), 0)
    owner, kind = lax.div(row, 8) + 1, lax.rem(row, 8)
    factor = jnp.where((kind == 1) | (kind == 5), s2, 1.0)
    factor = jnp.where(kind == 2, s3, factor)
    factor = jnp.where(kind == 3, s2 * s3, factor)
    inside = a3 == owner
    flat = (a3 == 0) & (a1 == owner)
    line = (a3 == 0) & (n1 == 0) & (a2 == owner)
    hit = jnp.where(kind < 4, inside.astype(F32), jnp.where(kind < 6, flat.astype(F32), line.astype(F32)))
    hit = jnp.where(kind == 7, 0.0, hit)
    left = hit * factor * g
    lane = lax.broadcasted_iota(jnp.int32, (32, count), 0)
    mine = atom + 1
    one, zero = jnp.ones((1, count), F32), jnp.zeros((1, count), F32)
    is1, is2 = (a1 == mine).astype(F32), (a2 == mine).astype(F32)
    no1, no2 = (n1 == 0).astype(F32), (n2 == 0).astype(F32)
    right = jnp.where(lane < N, is1 * (a2 == lane + 1).astype(F32), zero)
    right = jnp.where((lane >= 16) & (lane < 18), is1 * no2, right)
    right = jnp.where((lane >= 18) & (lane < 20), no1 * is2, right)
    right = jnp.where((lane >= 20) & (lane < 24), is2, right)
    right = jnp.where(lane == 24, no1 * no2, right)
    right = jnp.where((lane >= 25) & (lane < 27), no2, right)
    right = jnp.where((lane >= 27) & (lane < 29), one, right)
    right = jnp.concatenate([right, jnp.zeros((96, count), F32)]).astype(BF16)
    total = None
    for _ in range(3):
        piece = left.astype(BF16)
        left = left - piece.astype(F32)
        part = dot(piece, right, NT)
        total = part if total is None else total + part
    return total


def apply_green(t, gt):
    lanes = lax.broadcasted_iota(jnp.int32, (N, 128), 1)
    sign = jnp.where(lanes < Q, -1.0, 1.0)

    def swap(v):
        return jnp.concatenate([v[:, Q:], v[:, :Q]], axis=1)

    cc, cs, sc, ss = t[0:16], t[16:32], t[32:48], t[48:64]
    g0, g2, g3, g23 = (gt[0:16, k : k + 1] for k in range(4))
    xcc, xcs, xsc, xss = sign * swap(cc), sign * swap(cs), sign * swap(sc), sign * swap(ss)
    out = [
        g0 * cc - g2 * ss + g3 * xsc + g23 * xcs,
        g0 * cs + g2 * sc - g23 * xcc + g3 * xss,
        g0 * sc + g2 * cs - g3 * xcc + g23 * xss,
        g0 * ss - g2 * cc - g23 * xsc - g3 * xcs,
    ]
    e = t[64:80]
    r = lax.broadcasted_iota(jnp.int32, (N, 128), 0)
    h = [jnp.broadcast_to(gt[16:32, k : k + 1], (N, 128)) for k in range(8)]
    even = lax.rem(r, 2) == 0
    e0 = jnp.where(r < 4, h[0], jnp.where(r < 8, h[4], jnp.where(r == 8, h[0], jnp.where(r < 11, h[4], h[6]))))
    e0 = jnp.where(r < 13, e0, 0.0)
    e3 = jnp.where(r < 4, jnp.where(even, h[2], -h[2]), 0.0)
    e2 = jnp.where((r >= 4) & (r < 8), jnp.where(r < 6, -h[5], h[5]), 0.0)
    up = jnp.concatenate([e[1:], e[:1]], axis=0)
    down = jnp.concatenate([e[-1:], e[:-1]], axis=0)
    pair = jnp.where(even, up, down)
    out.append(e0 * e + e3 * (sign * swap(pair)) + e2 * pair)
    return jnp.concatenate(out, axis=0)


def pick(k, values):
    out = values[-1]
    for j in range(len(values) - 2, -1, -1):
        out = jnp.where(k == j, values[j], out)
    return out


def kernel(
    feat_in, species_in, coords_in, widx_in, green_in, embed_in, wc_in, wf_in, wp_in, wo_in, out,
    feat, species, coords, widx, green, embed, w_charge_t, w_feat, w_pot, w_out,
    cbuf, xbuf, gbuf, gsend, ebuf, zbuf, tabs, tabs_too, czs, tmain, tedge, wedge, thalf, tother, tsend, trecv, wall, wmain, wt, wflat,
    psend, precv, prelay, mixed, pre,
    in_sem, send_sem, cr_sem, xr_sem, gr_sem, th_sem, tr_sem, wr_sem, pr_sem, pq_sem,
):
    atom, wave = lax.axis_index("atom"), lax.axis_index("wave")
    here_y, here_x = lax.div(wave, 4), lax.rem(wave, 4)
    z, core = lax.div(atom, 2), lax.rem(atom, 2)
    partner = 2 * z + 1 - core
    ahead = 1 + 2 * core
    back = 3 - 2 * core

    def at(dy, dx):
        return lax.rem(here_y + dy, 4) * 4 + lax.rem(here_x + dx, 4)

    def opposite(dy, dx):
        return at(4 - dy, 4 - dx)

    PLACE_Y = (3, 1, 1, 3, 0, ahead, 0, back, 2, 1, 2, 3, 0, 2, 2)
    PLACE_X = (1, 1, 3, 3, ahead, 0, back, 0, 1, 2, 3, 2, 2, 0, 2)
    STEP_Y = (3, 0, 1, 0, 0, ahead, ahead)
    STEP_X = (0, 1, 0, 3, ahead, 0, ahead)
    corner = 1 + 2 * core

    def z_atom(dz, side):
        return 2 * lax.rem(z + dz, 8) + side

    def push(src, dst, ssem, rsem, axis, peer):
        return pltpu.make_async_remote_copy(
            src_ref=src, dst_ref=dst, send_sem=ssem, recv_sem=rsem,
            device_id={axis: peer}, device_id_type=pl.DeviceIdType.MESH,
        )

    def times(count, body, start=0):
        def step(k, carry):
            body(k)
            return carry

        lax.fori_loop(start, count, step, 0)

    barrier = pltpu.get_barrier_semaphore()

    def greet(axis, peer):
        pl.semaphore_signal(barrier, inc=1, device_id={axis: peer}, device_id_type=pl.DeviceIdType.MESH)

    for d in (4, 3, 5, 2, 6, 1, 7):
        greet("atom", z_atom(d, core))
    times(N, lambda d: greet("wave", at(lax.div(d, 4), lax.rem(d, 4))), 1)
    greet("atom", partner)

    loads = [
        pltpu.make_async_copy(src, dst, in_sem.at[k])
        for k, (src, dst) in enumerate(
            (
                (feat_in, feat), (species_in, species), (coords_in, coords), (embed_in, embed), (wc_in, w_charge_t),
                (widx_in, widx), (green_in, green), (wf_in, w_feat), (wp_in, w_pot), (wo_in, w_out),
            )
        )
    ]
    for load in loads:
        load.start()
    for load in loads[:5]:
        load.wait()

    hidden = feat[...].astype(F32)
    scale = lax.rsqrt(jnp.mean(hidden * hidden, axis=1, keepdims=True) + EPS)
    kinds = lax.broadcasted_iota(jnp.int32, (16, ATOMS), 0)
    onehot = (kinds == species[...]).astype(F32).astype(BF16)
    mixed_b = (hidden * scale + dot(onehot, embed[...], TN)).astype(BF16)
    mixed[...] = mixed_b
    cbuf[wave] = dot(w_charge_t[...], mixed_b, NT).astype(BF16)
    xbuf[wave] = coords[...]

    tmain[...] = jnp.zeros_like(tmain)
    tedge[...] = jnp.zeros_like(tedge)

    odd_wave = lax.rem(wave, 2)
    wave_sign = (1 - 2 * odd_wave).astype(F32)

    def prepare(slot, tabs, czs):
        place = xbuf[slot]
        j = lax.broadcasted_iota(jnp.int32, (HALF, ATOMS), 0).astype(F32) + 1.0
        tabs[0], tabs[1] = circle((2.0 * j - 0.5) * place[0:1])
        c, s = circle(j * place[1:2])
        c8, s8 = c[7:8], s[7:8]
        tabs[2], tabs[3] = c, c8 * c - s8 * s
        tabs[4], tabs[5] = s, s8 * c + c8 * s
        few = jnp.where(j == 1.0, 0.5 * place[0:1], (wave + 1).astype(F32) * place[2:3])
        tabs[6], tabs[7] = circle(few)
        hc, hs, zcw, zsw = tabs[6, 0:1, :], tabs[7, 0:1, :], tabs[6, 1:2, :], tabs[7, 1:2, :]
        rows = (hc * zcw, hc * zsw, hs * zcw, hs * zsw)
        zbuf[slot] = jnp.concatenate([*rows, jnp.zeros((4, ATOMS), F32)], axis=0)
        wide = cbuf[slot].astype(F32)
        for k in range(2):
            both = jnp.concatenate([rows[2 * k] * wide, rows[2 * k + 1] * wide], axis=0)
            czs[:, 128 * k : 128 * k + 128] = both.T.astype(BF16)

    def multiply(slot, tabs, czs):
        xc, xs = tabs[0], tabs[1]
        yc = jnp.concatenate([tabs[2], tabs[3]], axis=0)
        ys = jnp.concatenate([tabs[4], tabs[5]], axis=0)
        hc, hs = tabs[6, 0:1, :], tabs[7, 0:1, :]
        middle = lax.div(wave, 2)
        xcm, xsm = tabs[0, pl.ds(middle, 1), :], tabs[1, pl.ds(middle, 1), :]
        xcw = xcm * hc + wave_sign * (xsm * hs)
        xsw = xsm * hc - wave_sign * (xcm * hs)
        upper, lower = lax.div(wave, 8), lax.rem(wave, 8)
        ycw, ysw = tabs[2 + upper, pl.ds(lower, 1), :], tabs[4 + upper, pl.ds(lower, 1), :]
        for i in range(HALF):
            a, b = xc[i : i + 1], xs[i : i + 1]
            for k, part in enumerate((a * yc, a * ys, b * yc, b * ys)):
                ebuf[slot, 64 * i + N * k : 64 * i + N * (k + 1), :] = part.astype(BF16)
        r = lax.broadcasted_iota(jnp.int32, (N, ATOMS), 0)
        halves = jnp.where(r == 0, hc, jnp.where(r == 1, hs, 0.0))
        rest = jnp.zeros((N, ATOMS), F32)
        for k, row in enumerate((xcw, xsw, ycw, ysw)):
            rest = jnp.where(r == k + 1, row, rest)
        edge = (
            jnp.concatenate([xc, xs], axis=0), hc * yc, hc * ys, hs * yc, hs * ys, halves,
            xcw * yc, xsw * ys, xsw * yc, xcw * ys, rest,
        )
        for k, part in enumerate(edge):
            ebuf[slot, MAIN + N * k : MAIN + N * (k + 1), :] = part.astype(BF16)
        tmain[...] += dot(ebuf[slot, :LOW, :], czs[...])
        tedge[...] += dot(ebuf[slot, LOW:, :], cbuf[slot], NT)

    pl.semaphore_wait(barrier, 7 + 15 + 1)

    def c_copy(slot, peer):
        return push(cbuf.at[slot], cbuf.at[slot], send_sem.at[0], cr_sem.at[slot], "wave", peer)

    def x_copy(slot, peer):
        return push(xbuf.at[slot], xbuf.at[slot], send_sem.at[1], xr_sem.at[slot], "wave", peer)

    def send_on(slot, peer):
        x_copy(slot, peer).start()
        c_copy(slot, peer).start()

    for k in (1, 3, 0, 2, 4, 5, 6, 7):
        send_on(wave, at(PLACE_Y[k], PLACE_X[k]))

    for load in loads[5:]:
        load.wait()
    grid = green_rows(widx[0:1], widx[1:2], widx[2:3], green[...], atom)
    for k in range(N):
        gsend[k] = grid[8 * k : 8 * k + 8]
    gbuf[0] = gsend[wave]

    @functools.partial(times, N, start=1)
    def _(d):
        peer = at(lax.div(d, 4), lax.rem(d, 4))
        push(gsend.at[peer], gbuf.at[d], send_sem.at[2], gr_sem.at[0], "wave", peer).start()

    prepare(wave, tabs, czs)

    received = []
    for k in (1, 3, 0, 2, 4, 5, 6, 7, 9, 11, 8, 10, 12, 13, 14):
        code = PLACE_Y[k] + 4 * PLACE_X[k]
        if k < 6:
            code = code + 16 * STEP_Y[k] + 64 * STEP_X[k] + 256
        received.append(code)

    def receive(turn):
        code = pick(turn, received)
        slot = opposite(lax.rem(code, 4), lax.rem(lax.div(code, 4), 4))
        x_copy(slot, slot).wait_recv()
        c_copy(slot, slot).wait_recv()

        @pl.when(turn < 6)
        def _():
            send_on(slot, at(lax.rem(lax.div(code, 16), 4), lax.rem(lax.div(code, 64), 4)))

        @pl.when(turn == core)
        def _():
            send_on(slot, at(ahead, ahead))

        return slot

    def one(j, current):
        following = receive(j)
        for k in range(8):
            tabs_too[k] = tabs[k]
        multiply(current, tabs_too, czs)
        prepare(following, tabs, czs)
        return following

    current = lax.fori_loop(0, 15, one, wave)
    multiply(current, tabs, czs)

    low, high = slice(0, 128), slice(128, 256)
    xc, xs = slice(MAIN, MAIN + HALF), slice(MAIN + HALF, MAIN + N)
    for odd, sign in ((0, 1.0), (1, -1.0)):
        wedge[pl.ds(odd, HALF, stride=2), :] = tmain[xc, low] + sign * tmain[xs, high]
        wedge[pl.ds(N + odd, HALF, stride=2), :] = tmain[xs, low] - sign * tmain[xc, high]
    wedge[2 * N : 4 * N, :] = tmain[MAIN + N : MAIN + 3 * N, low] + tmain[MAIN + 3 * N : MAIN + 5 * N, high]
    wedge[4 * N :, :] = jnp.concatenate([tedge[...], jnp.zeros((5 * N, Q), F32)], axis=1)
    flat = tmain[MAIN + 5 * N : MAIN + 5 * N + 1, low] + tmain[MAIN + 5 * N + 1 : MAIN + 5 * N + 2, high]
    wedge[8 * N : 8 * N + 1, :] = flat

    def shard(ring, side):
        sign = (1 - 2 * side).astype(F32)
        c = pl.ds(pl.multiple_of(64 * ring, 64), 32)
        s = pl.ds(pl.multiple_of(64 * ring + 32, 32), 32)
        cosines = tmain[c, low] + sign * tmain[s, high]
        sines = tmain[s, low] - sign * tmain[c, high]
        edge = wedge[pl.ds(2 * ring + side, 8, stride=N), :]
        return jnp.concatenate([cosines, sines, edge, wedge[8 * N : 8 * N + 8, :]], axis=0)

    for k in range(8):
        thalf[k] = shard(jnp.int32(k), 1 - core).astype(BF16)
    half_copy = push(thalf, tother, th_sem.at[0], th_sem.at[1], "atom", partner)
    half_copy.start()
    pre[...] = dot(mixed[...], w_feat[...])
    push(gsend.at[0:15], gbuf.at[1:16], send_sem.at[2], gr_sem.at[0], "wave", wave).wait_recv()
    gsum = gbuf[0]
    for k in range(1, N):
        gsum = gsum + gbuf[k]
    columns = jnp.concatenate([gsum, jnp.zeros((120, 128), F32)], axis=0).T

    half_copy.wait_recv()

    def t_copy(d):
        return push(tsend.at[d], trecv.at[d], send_sem.at[3], tr_sem.at[0], "atom", z_atom(d, core))

    for d in (4, 3, 5, 2, 6, 1, 7):
        owner = lax.rem(z + d, 8)
        tsend[d] = (shard(owner, core) + tother[owner].astype(F32)).astype(BF16)
        t_copy(d).start()
    total = shard(z, core) + tother[z].astype(F32)

    all_shards = push(tsend.at[1:8], trecv.at[1:8], send_sem.at[3], tr_sem.at[0], "atom", atom)
    all_shards.wait_recv()
    for d in range(1, 8):
        total = total + trecv[d].astype(F32)
    wall[atom] = apply_green(total, columns).astype(BF16)

    def w_copy(slot, peer):
        return push(wall.at[slot], wall.at[slot], send_sem.at[4], wr_sem.at[slot], "atom", peer)

    for d in (4, 3, 5, 2, 6, 1, 7):
        w_copy(atom, z_atom(d, core)).start()
    w_copy(atom, partner).start()
    wmain[MAIN:, :] = jnp.zeros((128, 256), F32)

    def place_pair(d):
        ring = lax.rem(z + 8 - d, 8)
        w_copy(2 * ring + 1 - core, partner).wait_recv()
        first, second = wall[2 * ring].astype(F32), wall[2 * ring + 1].astype(F32)
        rows = pl.ds(pl.multiple_of(64 * ring, 64), 64)
        wmain[rows, low] = second[0:64] + first[0:64]
        wmain[rows, high] = jnp.concatenate([second[32:64] - first[32:64], first[0:32] - second[0:32]], axis=0)
        wedge[pl.ds(2 * ring, 8, stride=N), :] = first[64:72]
        wedge[pl.ds(2 * ring + 1, 8, stride=N), :] = second[64:72]

    order = (0, 1, 7, 2, 6, 3, 5, 4)
    for j, d in enumerate(order):
        if d:
            source = z_atom(8 - d, core)
            w_copy(source, partner).wait_recv()
            w_copy(source, partner).start()
        if j >= 2:
            place_pair(order[j - 2])
    for d in order[-2:]:
        place_pair(d)
    tail = wall[0, 72:80, :].astype(F32)
    fc, sc, fs, ss = (wedge[pl.ds(k, HALF, stride=2), :] for k in (0, 1, N, N + 1))
    wmain[xc, low], wmain[xc, high] = sc + fc, ss - fs
    wmain[xs, low], wmain[xs, high] = ss + fs, fc - sc
    wmain[MAIN + N : MAIN + 3 * N, low] = wedge[2 * N : 4 * N, :]
    wmain[MAIN + 3 * N : MAIN + 5 * N, high] = wedge[2 * N : 4 * N, :]
    wmain[MAIN + 5 * N : MAIN + 5 * N + 1, low] = tail[0:1]
    wmain[MAIN + 5 * N + 1 : MAIN + 5 * N + 2, high] = tail[0:1]
    for k in range(5):
        for half in (low, high):
            wt[half, 128 * k : 128 * k + 128] = wmain[128 * k : 128 * k + 128, half].T.astype(BF16)
    edges = jnp.concatenate([wedge[4 * N : 8 * N, :], tail, jnp.zeros((56, 128), F32)], axis=0).T
    column = lax.broadcasted_iota(jnp.int32, (Q, 128), 1)
    wflat[...] = jnp.where(column == 4 * N, 0.0, edges[:Q]).astype(BF16)

    prelay[7] = jnp.zeros((Q, ATOMS), BF16)

    def partial(slot):
        u = dot(wt[:, :LOW], ebuf[slot, :LOW, :])
        v = zbuf[slot]
        out = dot(wflat[:, : 5 * N], ebuf[slot, LOW:, :])
        for k in range(4):
            out = out + v[k : k + 1] * u[Q * k : Q * k + Q]
        return out

    def up_copy(k, peer):
        return push(psend.at[k], precv.at[k], send_sem.at[5], pr_sem.at[k], "wave", peer)

    def relay_copy(k, r, peer):
        return push(psend.at[k], prelay.at[r], send_sem.at[5], pq_sem.at[r], "wave", peer)

    across = 4 - corner
    turns = (14, 8 + corner, 8, 10, 8 + across, 12, 13, 6, 7, 0, 2, corner, across, 4, 5)

    @functools.partial(times, 15)
    def _(j):
        k = pick(j, turns)
        slot = opposite(pick(k, PLACE_Y), pick(k, PLACE_X))
        value = partial(slot)

        @pl.when(k < 6)
        def _():
            relay_copy(0, k, slot).wait_recv()

        @pl.when(k == corner)
        def _():
            relay_copy(0, 6, slot).wait_recv()

        value = value + prelay[jnp.where(k < 6, k, 7)].astype(F32)
        value = value + prelay[jnp.where(k == corner, 6, 7)].astype(F32)
        psend[k] = value.astype(BF16)

        @pl.when(k < 8)
        def _():
            up_copy(k, slot).start()

        @pl.when(k >= 8)
        def _():
            step = k - 8
            relay_copy(k, step, opposite(pick(step, STEP_Y), pick(step, STEP_X))).start()

    potential = partial(wave)
    for k in (6, 7, 0, 2, 1, 3, 4, 5):
        up_copy(k, wave).wait_recv()
        potential = potential + precv[k].astype(F32)
    potential_b = potential.T.astype(BF16)
    before = pre[...] + dot(potential_b, w_pot[...])
    activation = (before / (1.0 + jnp.exp(-before))).astype(BF16)
    out[...] = (feat[...].astype(F32) + dot(activation, w_out[...])).astype(BF16)

    half_copy.wait_send()
    all_shards.wait_send()
    push(cbuf.at[0:15], cbuf.at[0:15], send_sem.at[0], cr_sem.at[0], "wave", wave).wait_send()
    push(xbuf.at[0:15], xbuf.at[0:15], send_sem.at[1], xr_sem.at[0], "wave", wave).wait_send()
    push(gsend.at[0:15], gbuf.at[1:16], send_sem.at[2], gr_sem.at[0], "wave", wave).wait_send()
    push(wall.at[0:15], wall.at[0:15], send_sem.at[4], wr_sem.at[0], "atom", atom).wait_send()
    push(psend, psend, send_sem.at[5], pr_sem.at[0], "wave", wave).wait_send()


def shards(features, species, coords, wave_index, green, embed, w_charge, w_feat, w_pot, w_out):
    operands = (
        features, species.reshape(1, -1), coords, wave_index, green.reshape(1, -1),
        embed, w_charge.T, w_feat, w_pot, w_out,
    )
    return pl.pallas_call(
        kernel,
        out_shape=pltpu.VMEM(features.shape, BF16),
        in_specs=[pl.BlockSpec(memory_space=pl.ANY)] * 10,
        out_specs=pl.BlockSpec(memory_space=pltpu.VMEM),
        scratch_shapes=[pltpu.VMEM(v.shape, v.dtype) for v in operands]
        + [
            pltpu.VMEM((N, Q, ATOMS), BF16),
            pltpu.VMEM((N, 3, ATOMS), F32),
            pltpu.VMEM((N, 8, 128), F32),
            pltpu.VMEM((N, 8, 128), F32),
            pltpu.VMEM((N, ROWS, ATOMS), BF16),
            pltpu.VMEM((N, 8, ATOMS), F32),
            pltpu.VMEM((8, HALF, ATOMS), F32),
            pltpu.VMEM((8, HALF, ATOMS), F32),
            pltpu.VMEM((ATOMS, 256), BF16),
            pltpu.VMEM((LOW, 256), F32),
            pltpu.VMEM((5 * N, Q), F32),
            pltpu.VMEM((9 * N, 128), F32),
            pltpu.VMEM((8, SHARD, 128), BF16),
            pltpu.VMEM((8, SHARD, 128), BF16),
            pltpu.VMEM((8, SHARD, 128), BF16),
            pltpu.VMEM((8, SHARD, 128), BF16),
            pltpu.VMEM((N, SHARD, 128), BF16),
            pltpu.VMEM((MAIN + 128, 256), F32),
            pltpu.VMEM((256, MAIN + 128), BF16),
            pltpu.VMEM((Q, 128), BF16),
            pltpu.VMEM((15, Q, ATOMS), BF16),
            pltpu.VMEM((8, Q, ATOMS), BF16),
            pltpu.VMEM((8, Q, ATOMS), BF16),
            pltpu.VMEM((ATOMS, 128), BF16),
            pltpu.VMEM((ATOMS, 256), F32),
        ]
        + [pltpu.SemaphoreType.DMA((n,)) for n in (10, 6, N, N, 1, 2, 1, N, 8, 7)],
        compiler_params=pltpu.CompilerParams(
            collective_id=0, has_side_effects=True, vmem_limit_bytes=60 * 1024 * 1024
        ),
        name="ewald",
    )(*operands)


def solution(mesh):
    placed = (
        P(("atom", "wave"), None),
        P(("atom", "wave")),
        P(None, ("atom", "wave")),
        P(None, "wave"),
        P("wave"),
        P(),
        P(),
        P(),
        P(),
        P(),
    )
    return jax.shard_map(
        shards, mesh=mesh, in_specs=placed, out_specs=P(("atom", "wave"), None), check_vma=False
    )
```

```python
import functools

import jax
import jax.numpy as jnp
from jax import lax
from jax.experimental import pallas as pl
from jax.experimental.pallas import tpu as pltpu
from jax.sharding import PartitionSpec as P

EPS = 1e-06
N = 16
ATOMS = 512
Q = 64
HALF = N // 2
MAIN = 64 * HALF
LOW = MAIN + 6 * N
ROWS = LOW + 5 * N
SHARD = 80
COS = (0.9999999890590228, -19.739204499453827, 64.9391174598908, -85.45013953079768, 60.16763095026347, -25.967599245923736, 6.52865815775625)
SIN = (6.2831853025115025, -41.341700405317205, 81.60513138578321, -76.70301535364746, 42.02592698447418, -14.8998466635365, 3.2381375046186873)
F32 = jnp.float32
BF16 = jnp.bfloat16
NT = (((1,), (1,)), ((), ()))
TN = (((0,), (0,)), ((), ()))


def dot(a, b, dims=(((1,), (0,)), ((), ()))):
    return lax.dot_general(a, b, dims, preferred_element_type=F32)


def poly(u, coeffs):
    total = jnp.full_like(u, coeffs[-1])
    for c in coeffs[-2::-1]:
        total = total * u + c
    return total


def circle(turns):
    r = turns - jnp.round(turns)
    u = r * r
    return poly(u, COS), r * poly(u, SIN)


def green_rows(n1, n2, n3, g, atom, key=None):
    count = n1.shape[1]
    first = jnp.where(n1 != 0, n1, jnp.where(n2 != 0, n2, n3))
    s = jnp.where(first < 0, -1, 1)
    a1, a2, a3 = jnp.abs(n1), jnp.abs(n2), jnp.abs(n3)
    s2 = jnp.where(n2 * s < 0, -1.0, 1.0)
    s3 = jnp.where(n3 * s < 0, -1.0, 1.0)
    row = lax.broadcasted_iota(jnp.int32, (8 * N, count), 0)
    owner, kind = lax.div(row, 8) + 1, lax.rem(row, 8)
    factor = jnp.where((kind == 1) | (kind == 5), s2, 1.0)
    factor = jnp.where(kind == 2, s3, factor)
    factor = jnp.where(kind == 3, s2 * s3, factor)
    inside = a3 == owner
    flat = (a3 == 0) & (a1 == owner)
    line = (a3 == 0) & (n1 == 0) & (a2 == owner)
    hit = jnp.where(kind < 4, inside.astype(F32), jnp.where(kind < 6, flat.astype(F32), line.astype(F32)))
    hit = jnp.where(kind == 7, 0.0, hit)
    left = hit * factor * g
    lane = lax.broadcasted_iota(jnp.int32, (32, count), 0)
    mine = atom + 1
    one, zero = jnp.ones((1, count), F32), jnp.zeros((1, count), F32)
    is1, is2 = (a1 == mine).astype(F32), (a2 == mine).astype(F32)
    no1, no2 = (n1 == 0).astype(F32), (n2 == 0).astype(F32)
    right = jnp.where(lane < N, is1 * (a2 == lane + 1).astype(F32), zero)
    right = jnp.where((lane >= 16) & (lane < 18), is1 * no2, right)
    right = jnp.where((lane >= 18) & (lane < 20), no1 * is2, right)
    right = jnp.where((lane >= 20) & (lane < 24), is2, right)
    right = jnp.where(lane == 24, no1 * no2, right)
    right = jnp.where((lane >= 25) & (lane < 27), no2, right)
    right = jnp.where((lane >= 27) & (lane < 29), one, right)
    right = jnp.concatenate([right, jnp.zeros((96, count), F32)]).astype(BF16)
    total = None
    for _ in range(3):
        piece = left.astype(BF16)
        left = left - piece.astype(F32)
        part = dot(piece, right, NT)
        total = part if total is None else total + part
    return total


def apply_green(t, gt):
    lanes = lax.broadcasted_iota(jnp.int32, (N, 128), 1)
    sign = jnp.where(lanes < Q, -1.0, 1.0)

    def swap(v):
        return jnp.concatenate([v[:, Q:], v[:, :Q]], axis=1)

    cc, cs, sc, ss = t[0:16], t[16:32], t[32:48], t[48:64]
    g0, g2, g3, g23 = (gt[0:16, k : k + 1] for k in range(4))
    xcc, xcs, xsc, xss = sign * swap(cc), sign * swap(cs), sign * swap(sc), sign * swap(ss)
    out = [
        g0 * cc - g2 * ss + g3 * xsc + g23 * xcs,
        g0 * cs + g2 * sc - g23 * xcc + g3 * xss,
        g0 * sc + g2 * cs - g3 * xcc + g23 * xss,
        g0 * ss - g2 * cc - g23 * xsc - g3 * xcs,
    ]
    e = t[64:80]
    r = lax.broadcasted_iota(jnp.int32, (N, 128), 0)
    h = [jnp.broadcast_to(gt[16:32, k : k + 1], (N, 128)) for k in range(8)]
    even = lax.rem(r, 2) == 0
    e0 = jnp.where(r < 4, h[0], jnp.where(r < 8, h[4], jnp.where(r == 8, h[0], jnp.where(r < 11, h[4], h[6]))))
    e0 = jnp.where(r < 13, e0, 0.0)
    e3 = jnp.where(r < 4, jnp.where(even, h[2], -h[2]), 0.0)
    e2 = jnp.where((r >= 4) & (r < 8), jnp.where(r < 6, -h[5], h[5]), 0.0)
    up = jnp.concatenate([e[1:], e[:1]], axis=0)
    down = jnp.concatenate([e[-1:], e[:-1]], axis=0)
    pair = jnp.where(even, up, down)
    out.append(e0 * e + e3 * (sign * swap(pair)) + e2 * pair)
    return jnp.concatenate(out, axis=0)


def pick(k, values):
    out = values[-1]
    for j in range(len(values) - 2, -1, -1):
        out = jnp.where(k == j, values[j], out)
    return out


def kernel(
    feat_in, species_in, coords_in, widx_in, green_in, embed_in, wc_in, wf_in, wp_in, wo_in, out,
    feat, species, coords, widx, green, embed, w_charge_t, w_feat, w_pot, w_out,
    cbuf, xbuf, gbuf, gsend, ebuf, zbuf, tabs, tabs_too, czs, tmain, tedge, wedge, thalf, tother, tsend, trecv, wall, wmain, wt, wflat,
    psend, precv, prelay, mixed, pre,
    in_sem, send_sem, cr_sem, xr_sem, gr_sem, th_sem, tr_sem, wr_sem, pr_sem, pq_sem, chain_sem,
):
    atom, wave = lax.axis_index("atom"), lax.axis_index("wave")
    here_y, here_x = lax.div(wave, 4), lax.rem(wave, 4)
    z, core = lax.div(atom, 2), lax.rem(atom, 2)
    partner = 2 * z + 1 - core
    ahead = 1 + 2 * core
    back = 3 - 2 * core

    def at(dy, dx):
        return lax.rem(here_y + dy, 4) * 4 + lax.rem(here_x + dx, 4)

    def opposite(dy, dx):
        return at(4 - dy, 4 - dx)

    PLACE_Y = (3, 1, 1, 3, 0, ahead, 0, back, 2, 1, 2, 3, 0, 2, 2)
    PLACE_X = (1, 1, 3, 3, ahead, 0, back, 0, 1, 2, 3, 2, 2, 0, 2)
    STEP_Y = (3, 0, 1, 0, 0, ahead, ahead)
    STEP_X = (0, 1, 0, 3, ahead, 0, ahead)
    corner = 1 + 2 * core

    def z_atom(dz, side):
        return 2 * lax.rem(z + dz, 8) + side

    def push(src, dst, ssem, rsem, axis, peer):
        return pltpu.make_async_remote_copy(
            src_ref=src, dst_ref=dst, send_sem=ssem, recv_sem=rsem,
            device_id={axis: peer}, device_id_type=pl.DeviceIdType.MESH,
        )

    def times(count, body, start=0):
        def step(k, carry):
            body(k)
            return carry

        lax.fori_loop(start, count, step, 0)

    barrier = pltpu.get_barrier_semaphore()

    def greet(axis, peer):
        pl.semaphore_signal(barrier, inc=1, device_id={axis: peer}, device_id_type=pl.DeviceIdType.MESH)

    for k in range(8):
        greet("wave", at(PLACE_Y[k], PLACE_X[k]))
    for d in (1, 7):
        greet("atom", z_atom(d, core))
    greet("atom", partner)

    def pass_on(k, d):
        peer = {"atom": z_atom(d, core)}
        pl.semaphore_signal(chain_sem.at[k], inc=1, device_id=peer, device_id_type=pl.DeviceIdType.MESH)

    loads = [
        pltpu.make_async_copy(src, dst, in_sem.at[k])
        for k, (src, dst) in enumerate(
            (
                (feat_in, feat), (species_in, species), (coords_in, coords), (embed_in, embed), (wc_in, w_charge_t),
                (widx_in, widx), (green_in, green), (wf_in, w_feat), (wp_in, w_pot), (wo_in, w_out),
            )
        )
    ]
    for load in loads:
        load.start()
    for load in loads[:5]:
        load.wait()

    hidden = feat[...].astype(F32)
    scale = lax.rsqrt(jnp.mean(hidden * hidden, axis=1, keepdims=True) + EPS)
    kinds = lax.broadcasted_iota(jnp.int32, (16, ATOMS), 0)
    onehot = (kinds == species[...]).astype(F32).astype(BF16)
    mixed_b = (hidden * scale + dot(onehot, embed[...], TN)).astype(BF16)
    mixed[...] = mixed_b
    cbuf[wave] = dot(w_charge_t[...], mixed_b, NT).astype(BF16)
    xbuf[wave] = coords[...]

    tmain[...] = jnp.zeros_like(tmain)
    tedge[...] = jnp.zeros_like(tedge)

    odd_wave = lax.rem(wave, 2)
    wave_sign = (1 - 2 * odd_wave).astype(F32)

    def prepare(slot, tabs, czs):
        place = xbuf[slot]
        j = lax.broadcasted_iota(jnp.int32, (HALF, ATOMS), 0).astype(F32) + 1.0
        tabs[0], tabs[1] = circle((2.0 * j - 0.5) * place[0:1])
        c, s = circle(j * place[1:2])
        c8, s8 = c[7:8], s[7:8]
        tabs[2], tabs[3] = c, c8 * c - s8 * s
        tabs[4], tabs[5] = s, s8 * c + c8 * s
        few = jnp.where(j == 1.0, 0.5 * place[0:1], (wave + 1).astype(F32) * place[2:3])
        tabs[6], tabs[7] = circle(few)
        hc, hs, zcw, zsw = tabs[6, 0:1, :], tabs[7, 0:1, :], tabs[6, 1:2, :], tabs[7, 1:2, :]
        rows = (hc * zcw, hc * zsw, hs * zcw, hs * zsw)
        zbuf[slot] = jnp.concatenate([*rows, jnp.zeros((4, ATOMS), F32)], axis=0)
        wide = cbuf[slot].astype(F32)
        for k in range(2):
            both = jnp.concatenate([rows[2 * k] * wide, rows[2 * k + 1] * wide], axis=0)
            czs[:, 128 * k : 128 * k + 128] = both.T.astype(BF16)

    def multiply(slot, tabs, czs):
        xc, xs = tabs[0], tabs[1]
        yc = jnp.concatenate([tabs[2], tabs[3]], axis=0)
        ys = jnp.concatenate([tabs[4], tabs[5]], axis=0)
        hc, hs = tabs[6, 0:1, :], tabs[7, 0:1, :]
        middle = lax.div(wave, 2)
        xcm, xsm = tabs[0, pl.ds(middle, 1), :], tabs[1, pl.ds(middle, 1), :]
        xcw = xcm * hc + wave_sign * (xsm * hs)
        xsw = xsm * hc - wave_sign * (xcm * hs)
        upper, lower = lax.div(wave, 8), lax.rem(wave, 8)
        ycw, ysw = tabs[2 + upper, pl.ds(lower, 1), :], tabs[4 + upper, pl.ds(lower, 1), :]
        for i in range(HALF):
            a, b = xc[i : i + 1], xs[i : i + 1]
            for k, part in enumerate((a * yc, a * ys, b * yc, b * ys)):
                ebuf[slot, 64 * i + N * k : 64 * i + N * (k + 1), :] = part.astype(BF16)
        r = lax.broadcasted_iota(jnp.int32, (N, ATOMS), 0)
        halves = jnp.where(r == 0, hc, jnp.where(r == 1, hs, 0.0))
        rest = jnp.zeros((N, ATOMS), F32)
        for k, row in enumerate((xcw, xsw, ycw, ysw)):
            rest = jnp.where(r == k + 1, row, rest)
        edge = (
            jnp.concatenate([xc, xs], axis=0), hc * yc, hc * ys, hs * yc, hs * ys, halves,
            xcw * yc, xsw * ys, xsw * yc, xcw * ys, rest,
        )
        for k, part in enumerate(edge):
            ebuf[slot, MAIN + N * k : MAIN + N * (k + 1), :] = part.astype(BF16)
        tmain[...] += dot(ebuf[slot, :LOW, :], czs[...])
        tedge[...] += dot(ebuf[slot, LOW:, :], cbuf[slot], NT)

    pl.semaphore_wait(barrier, 8 + 2 + 1)

    def c_copy(slot, peer):
        return push(cbuf.at[slot], cbuf.at[slot], send_sem.at[0], cr_sem.at[slot], "wave", peer)

    def x_copy(slot, peer):
        return push(xbuf.at[slot], xbuf.at[slot], send_sem.at[1], xr_sem.at[slot], "wave", peer)

    def send_on(slot, peer):
        x_copy(slot, peer).start()
        c_copy(slot, peer).start()

    for k in (1, 3, 0, 2, 4, 5, 6, 7):
        send_on(wave, at(PLACE_Y[k], PLACE_X[k]))

    for load in loads[5:]:
        load.wait()
    grid = green_rows(widx[0:1], widx[1:2], widx[2:3], green[...], atom)
    for k in range(N):
        gsend[k] = grid[8 * k : 8 * k + 8]
    gbuf[0] = gsend[wave]

    pass_on(0, 1)
    pass_on(1, 7)
    prepare(wave, tabs, czs)

    received = []
    for k in (1, 3, 0, 2, 4, 5, 6, 7, 9, 11, 8, 10, 12, 13, 14):
        code = PLACE_Y[k] + 4 * PLACE_X[k]
        if k < 6:
            code = code + 16 * STEP_Y[k] + 64 * STEP_X[k] + 256
        received.append(code)

    def receive(turn):
        code = pick(turn, received)
        slot = opposite(lax.rem(code, 4), lax.rem(lax.div(code, 4), 4))
        x_copy(slot, slot).wait_recv()
        c_copy(slot, slot).wait_recv()

        @pl.when(turn < 6)
        def _():
            send_on(slot, at(lax.rem(lax.div(code, 16), 4), lax.rem(lax.div(code, 64), 4)))

        @pl.when(turn == core)
        def _():
            send_on(slot, at(ahead, ahead))

        return slot

    def one(j, current):
        following = receive(j)
        for k in range(8):
            tabs_too[k] = tabs[k]
        multiply(current, tabs_too, czs)
        prepare(following, tabs, czs)
        return following

    current = lax.fori_loop(0, 8, one, wave)
    for k in (0, 1):
        pl.semaphore_wait(chain_sem.at[k], 1)
    pass_on(2, 1)
    pass_on(3, 7)
    current = lax.fori_loop(8, 15, one, current)
    for k in (2, 3):
        pl.semaphore_wait(chain_sem.at[k], 1)
    pass_on(4, 1)
    multiply(current, tabs, czs)

    low, high = slice(0, 128), slice(128, 256)
    xc, xs = slice(MAIN, MAIN + HALF), slice(MAIN + HALF, MAIN + N)
    for odd, sign in ((0, 1.0), (1, -1.0)):
        wedge[pl.ds(odd, HALF, stride=2), :] = tmain[xc, low] + sign * tmain[xs, high]
        wedge[pl.ds(N + odd, HALF, stride=2), :] = tmain[xs, low] - sign * tmain[xc, high]
    wedge[2 * N : 4 * N, :] = tmain[MAIN + N : MAIN + 3 * N, low] + tmain[MAIN + 3 * N : MAIN + 5 * N, high]
    wedge[4 * N :, :] = jnp.concatenate([tedge[...], jnp.zeros((5 * N, Q), F32)], axis=1)
    flat = tmain[MAIN + 5 * N : MAIN + 5 * N + 1, low] + tmain[MAIN + 5 * N + 1 : MAIN + 5 * N + 2, high]
    wedge[8 * N : 8 * N + 1, :] = flat

    def shard(ring, side):
        sign = (1 - 2 * side).astype(F32)
        c = pl.ds(pl.multiple_of(64 * ring, 64), 32)
        s = pl.ds(pl.multiple_of(64 * ring + 32, 32), 32)
        cosines = tmain[c, low] + sign * tmain[s, high]
        sines = tmain[s, low] - sign * tmain[c, high]
        edge = wedge[pl.ds(2 * ring + side, 8, stride=N), :]
        return jnp.concatenate([cosines, sines, edge, wedge[8 * N : 8 * N + 8, :]], axis=0)

    for k in range(8):
        thalf[k] = shard(jnp.int32(k), 1 - core).astype(BF16)
    half_copy = push(thalf, tother, th_sem.at[0], th_sem.at[1], "atom", partner)
    half_copy.start()

    @functools.partial(times, N, start=1)
    def _(d):
        peer = at(lax.div(d, 4), lax.rem(d, 4))
        push(gsend.at[peer], gbuf.at[d], send_sem.at[2], gr_sem.at[0], "wave", peer).start()

    half_copy.wait_recv()
    pl.semaphore_wait(chain_sem.at[4], 1)

    def t_copy(d):
        return push(tsend.at[d], trecv.at[d], send_sem.at[3], tr_sem.at[0], "atom", z_atom(d, core))

    for d in (4, 3, 5, 2, 6, 1, 7):
        owner = lax.rem(z + d, 8)
        tsend[d] = (shard(owner, core) + tother[owner].astype(F32)).astype(BF16)
        t_copy(d).start()
    total = shard(z, core) + tother[z].astype(F32)
    pre[...] = dot(mixed[...], w_feat[...])
    push(gsend.at[0:15], gbuf.at[1:16], send_sem.at[2], gr_sem.at[0], "wave", wave).wait_recv()
    gsum = gbuf[0]
    for k in range(1, N):
        gsum = gsum + gbuf[k]
    columns = jnp.concatenate([gsum, jnp.zeros((120, 128), F32)], axis=0).T


    all_shards = push(tsend.at[1:8], trecv.at[1:8], send_sem.at[3], tr_sem.at[0], "atom", atom)
    all_shards.wait_recv()
    for d in range(1, 8):
        total = total + trecv[d].astype(F32)
    wall[atom] = apply_green(total, columns).astype(BF16)

    def w_copy(slot, peer):
        return push(wall.at[slot], wall.at[slot], send_sem.at[4], wr_sem.at[slot], "atom", peer)

    for d in (4, 3, 5, 2, 6, 1, 7):
        w_copy(atom, z_atom(d, core)).start()
    w_copy(atom, partner).start()
    wmain[MAIN:, :] = jnp.zeros((128, 256), F32)

    def place_pair(d):
        ring = lax.rem(z + 8 - d, 8)
        w_copy(2 * ring + 1 - core, partner).wait_recv()
        first, second = wall[2 * ring].astype(F32), wall[2 * ring + 1].astype(F32)
        rows = pl.ds(pl.multiple_of(64 * ring, 64), 64)
        wmain[rows, low] = second[0:64] + first[0:64]
        wmain[rows, high] = jnp.concatenate([second[32:64] - first[32:64], first[0:32] - second[0:32]], axis=0)
        wedge[pl.ds(2 * ring, 8, stride=N), :] = first[64:72]
        wedge[pl.ds(2 * ring + 1, 8, stride=N), :] = second[64:72]

    order = (0, 1, 7, 2, 6, 3, 5, 4)
    for j, d in enumerate(order):
        if d:
            source = z_atom(8 - d, core)
            w_copy(source, partner).wait_recv()
            w_copy(source, partner).start()
        if j >= 2:
            place_pair(order[j - 2])
    for d in order[-2:]:
        place_pair(d)
    tail = wall[0, 72:80, :].astype(F32)
    fc, sc, fs, ss = (wedge[pl.ds(k, HALF, stride=2), :] for k in (0, 1, N, N + 1))
    wmain[xc, low], wmain[xc, high] = sc + fc, ss - fs
    wmain[xs, low], wmain[xs, high] = ss + fs, fc - sc
    wmain[MAIN + N : MAIN + 3 * N, low] = wedge[2 * N : 4 * N, :]
    wmain[MAIN + 3 * N : MAIN + 5 * N, high] = wedge[2 * N : 4 * N, :]
    wmain[MAIN + 5 * N : MAIN + 5 * N + 1, low] = tail[0:1]
    wmain[MAIN + 5 * N + 1 : MAIN + 5 * N + 2, high] = tail[0:1]
    for k in range(5):
        for half in (low, high):
            wt[half, 128 * k : 128 * k + 128] = wmain[128 * k : 128 * k + 128, half].T.astype(BF16)
    edges = jnp.concatenate([wedge[4 * N : 8 * N, :], tail, jnp.zeros((56, 128), F32)], axis=0).T
    column = lax.broadcasted_iota(jnp.int32, (Q, 128), 1)
    wflat[...] = jnp.where(column == 4 * N, 0.0, edges[:Q]).astype(BF16)

    prelay[7] = jnp.zeros((Q, ATOMS), BF16)

    def partial(slot):
        u = dot(wt[:, :LOW], ebuf[slot, :LOW, :])
        v = zbuf[slot]
        out = dot(wflat[:, : 5 * N], ebuf[slot, LOW:, :])
        for k in range(4):
            out = out + v[k : k + 1] * u[Q * k : Q * k + Q]
        return out

    def up_copy(k, peer):
        return push(psend.at[k], precv.at[k], send_sem.at[5], pr_sem.at[k], "wave", peer)

    def relay_copy(k, r, peer):
        return push(psend.at[k], prelay.at[r], send_sem.at[5], pq_sem.at[r], "wave", peer)

    across = 4 - corner
    turns = (14, 8 + corner, 8, 10, 8 + across, 12, 13, 6, 7, 0, 2, corner, across, 4, 5)

    @functools.partial(times, 15)
    def _(j):
        k = pick(j, turns)
        slot = opposite(pick(k, PLACE_Y), pick(k, PLACE_X))
        value = partial(slot)

        @pl.when(k < 6)
        def _():
            relay_copy(0, k, slot).wait_recv()

        @pl.when(k == corner)
        def _():
            relay_copy(0, 6, slot).wait_recv()

        value = value + prelay[jnp.where(k < 6, k, 7)].astype(F32)
        value = value + prelay[jnp.where(k == corner, 6, 7)].astype(F32)
        psend[k] = value.astype(BF16)

        @pl.when(k < 8)
        def _():
            up_copy(k, slot).start()

        @pl.when(k >= 8)
        def _():
            step = k - 8
            relay_copy(k, step, opposite(pick(step, STEP_Y), pick(step, STEP_X))).start()

    potential = partial(wave)
    for k in (6, 7, 0, 2, 1, 3, 4, 5):
        up_copy(k, wave).wait_recv()
        potential = potential + precv[k].astype(F32)
    potential_b = potential.T.astype(BF16)
    before = pre[...] + dot(potential_b, w_pot[...])
    activation = (before / (1.0 + jnp.exp(-before))).astype(BF16)
    out[...] = (feat[...].astype(F32) + dot(activation, w_out[...])).astype(BF16)

    half_copy.wait_send()
    all_shards.wait_send()
    push(cbuf.at[0:15], cbuf.at[0:15], send_sem.at[0], cr_sem.at[0], "wave", wave).wait_send()
    push(xbuf.at[0:15], xbuf.at[0:15], send_sem.at[1], xr_sem.at[0], "wave", wave).wait_send()
    push(gsend.at[0:15], gbuf.at[1:16], send_sem.at[2], gr_sem.at[0], "wave", wave).wait_send()
    push(wall.at[0:15], wall.at[0:15], send_sem.at[4], wr_sem.at[0], "atom", atom).wait_send()
    push(psend, psend, send_sem.at[5], pr_sem.at[0], "wave", wave).wait_send()


def shards(features, species, coords, wave_index, green, embed, w_charge, w_feat, w_pot, w_out):
    operands = (
        features, species.reshape(1, -1), coords, wave_index, green.reshape(1, -1),
        embed, w_charge.T, w_feat, w_pot, w_out,
    )
    return pl.pallas_call(
        kernel,
        out_shape=pltpu.VMEM(features.shape, BF16),
        in_specs=[pl.BlockSpec(memory_space=pl.ANY)] * 10,
        out_specs=pl.BlockSpec(memory_space=pltpu.VMEM),
        scratch_shapes=[pltpu.VMEM(v.shape, v.dtype) for v in operands]
        + [
            pltpu.VMEM((N, Q, ATOMS), BF16),
            pltpu.VMEM((N, 3, ATOMS), F32),
            pltpu.VMEM((N, 8, 128), F32),
            pltpu.VMEM((N, 8, 128), F32),
            pltpu.VMEM((N, ROWS, ATOMS), BF16),
            pltpu.VMEM((N, 8, ATOMS), F32),
            pltpu.VMEM((8, HALF, ATOMS), F32),
            pltpu.VMEM((8, HALF, ATOMS), F32),
            pltpu.VMEM((ATOMS, 256), BF16),
            pltpu.VMEM((LOW, 256), F32),
            pltpu.VMEM((5 * N, Q), F32),
            pltpu.VMEM((9 * N, 128), F32),
            pltpu.VMEM((8, SHARD, 128), BF16),
            pltpu.VMEM((8, SHARD, 128), BF16),
            pltpu.VMEM((8, SHARD, 128), BF16),
            pltpu.VMEM((8, SHARD, 128), BF16),
            pltpu.VMEM((N, SHARD, 128), BF16),
            pltpu.VMEM((MAIN + 128, 256), F32),
            pltpu.VMEM((256, MAIN + 128), BF16),
            pltpu.VMEM((Q, 128), BF16),
            pltpu.VMEM((15, Q, ATOMS), BF16),
            pltpu.VMEM((8, Q, ATOMS), BF16),
            pltpu.VMEM((8, Q, ATOMS), BF16),
            pltpu.VMEM((ATOMS, 128), BF16),
            pltpu.VMEM((ATOMS, 256), F32),
        ]
        + [pltpu.SemaphoreType.DMA((n,)) for n in (10, 6, N, N, 1, 2, 1, N, 8, 7)]
        + [pltpu.SemaphoreType.REGULAR((5,))],
        compiler_params=pltpu.CompilerParams(
            collective_id=0, has_side_effects=True, vmem_limit_bytes=60 * 1024 * 1024
        ),
        name="ewald",
    )(*operands)


def solution(mesh):
    placed = (
        P(("atom", "wave"), None),
        P(("atom", "wave")),
        P(None, ("atom", "wave")),
        P(None, "wave"),
        P("wave"),
        P(),
        P(),
        P(),
        P(),
        P(),
    )
    return jax.shard_map(
        shards, mesh=mesh, in_specs=placed, out_specs=P(("atom", "wave"), None), check_vma=False
    )
```

```python
import functools

import jax
import jax.numpy as jnp
from jax import lax
from jax.experimental import pallas as pl
from jax.experimental.pallas import tpu as pltpu
from jax.sharding import PartitionSpec as P

EPS = 1e-06
N = 16
ATOMS = 512
Q = 64
HALF = N // 2
MAIN = 64 * HALF
LOW = MAIN + 6 * N
ROWS = LOW + 5 * N
SHARD = 80
COS = (0.9999999890590228, -19.739204499453827, 64.9391174598908, -85.45013953079768, 60.16763095026347, -25.967599245923736, 6.52865815775625)
SIN = (6.2831853025115025, -41.341700405317205, 81.60513138578321, -76.70301535364746, 42.02592698447418, -14.8998466635365, 3.2381375046186873)
F32 = jnp.float32
BF16 = jnp.bfloat16
NT = (((1,), (1,)), ((), ()))
TN = (((0,), (0,)), ((), ()))


def dot(a, b, dims=(((1,), (0,)), ((), ()))):
    return lax.dot_general(a, b, dims, preferred_element_type=F32)


def poly(u, coeffs):
    total = jnp.full_like(u, coeffs[-1])
    for c in coeffs[-2::-1]:
        total = total * u + c
    return total


def circle(turns):
    r = turns - jnp.round(turns)
    u = r * r
    return poly(u, COS), r * poly(u, SIN)


def green_rows(n1, n2, n3, g, atom, key=None):
    count = n1.shape[1]
    first = jnp.where(n1 != 0, n1, jnp.where(n2 != 0, n2, n3))
    s = jnp.where(first < 0, -1, 1)
    a1, a2, a3 = jnp.abs(n1), jnp.abs(n2), jnp.abs(n3)
    s2 = jnp.where(n2 * s < 0, -1.0, 1.0)
    s3 = jnp.where(n3 * s < 0, -1.0, 1.0)
    row = lax.broadcasted_iota(jnp.int32, (8 * N, count), 0)
    owner, kind = lax.div(row, 8) + 1, lax.rem(row, 8)
    factor = jnp.where((kind == 1) | (kind == 5), s2, 1.0)
    factor = jnp.where(kind == 2, s3, factor)
    factor = jnp.where(kind == 3, s2 * s3, factor)
    inside = a3 == owner
    flat = (a3 == 0) & (a1 == owner)
    line = (a3 == 0) & (n1 == 0) & (a2 == owner)
    hit = jnp.where(kind < 4, inside.astype(F32), jnp.where(kind < 6, flat.astype(F32), line.astype(F32)))
    hit = jnp.where(kind == 7, 0.0, hit)
    left = hit * factor * g
    lane = lax.broadcasted_iota(jnp.int32, (32, count), 0)
    mine = atom + 1
    one, zero = jnp.ones((1, count), F32), jnp.zeros((1, count), F32)
    is1, is2 = (a1 == mine).astype(F32), (a2 == mine).astype(F32)
    no1, no2 = (n1 == 0).astype(F32), (n2 == 0).astype(F32)
    right = jnp.where(lane < N, is1 * (a2 == lane + 1).astype(F32), zero)
    right = jnp.where((lane >= 16) & (lane < 18), is1 * no2, right)
    right = jnp.where((lane >= 18) & (lane < 20), no1 * is2, right)
    right = jnp.where((lane >= 20) & (lane < 24), is2, right)
    right = jnp.where(lane == 24, no1 * no2, right)
    right = jnp.where((lane >= 25) & (lane < 27), no2, right)
    right = jnp.where((lane >= 27) & (lane < 29), one, right)
    right = jnp.concatenate([right, jnp.zeros((96, count), F32)]).astype(BF16)
    total = None
    for _ in range(3):
        piece = left.astype(BF16)
        left = left - piece.astype(F32)
        part = dot(piece, right, NT)
        total = part if total is None else total + part
    return total


def apply_green(t, gt):
    lanes = lax.broadcasted_iota(jnp.int32, (N, 128), 1)
    sign = jnp.where(lanes < Q, -1.0, 1.0)

    def swap(v):
        return jnp.concatenate([v[:, Q:], v[:, :Q]], axis=1)

    cc, cs, sc, ss = t[0:16], t[16:32], t[32:48], t[48:64]
    g0, g2, g3, g23 = (gt[0:16, k : k + 1] for k in range(4))
    xcc, xcs, xsc, xss = sign * swap(cc), sign * swap(cs), sign * swap(sc), sign * swap(ss)
    out = [
        g0 * cc - g2 * ss + g3 * xsc + g23 * xcs,
        g0 * cs + g2 * sc - g23 * xcc + g3 * xss,
        g0 * sc + g2 * cs - g3 * xcc + g23 * xss,
        g0 * ss - g2 * cc - g23 * xsc - g3 * xcs,
    ]
    e = t[64:80]
    r = lax.broadcasted_iota(jnp.int32, (N, 128), 0)
    h = [jnp.broadcast_to(gt[16:32, k : k + 1], (N, 128)) for k in range(8)]
    even = lax.rem(r, 2) == 0
    e0 = jnp.where(r < 4, h[0], jnp.where(r < 8, h[4], jnp.where(r == 8, h[0], jnp.where(r < 11, h[4], h[6]))))
    e0 = jnp.where(r < 13, e0, 0.0)
    e3 = jnp.where(r < 4, jnp.where(even, h[2], -h[2]), 0.0)
    e2 = jnp.where((r >= 4) & (r < 8), jnp.where(r < 6, -h[5], h[5]), 0.0)
    up = jnp.concatenate([e[1:], e[:1]], axis=0)
    down = jnp.concatenate([e[-1:], e[:-1]], axis=0)
    pair = jnp.where(even, up, down)
    out.append(e0 * e + e3 * (sign * swap(pair)) + e2 * pair)
    return jnp.concatenate(out, axis=0)


def pick(k, values):
    out = values[-1]
    for j in range(len(values) - 2, -1, -1):
        out = jnp.where(k == j, values[j], out)
    return out


def kernel(
    feat_in, species_in, coords_in, widx_in, green_in, embed_in, wc_in, wf_in, wp_in, wo_in, out,
    feat, species, coords, widx, green, embed, w_charge_t, w_feat, w_pot, w_out,
    cbuf, xbuf, gbuf, gsend, ebuf, zbuf, tabs, tabs_too, czs, tmain, tedge, wedge, thalf, tother, tsend, trecv, wall, wmain, wt, wflat,
    psend, precv, prelay, mixed, pre,
    in_sem, send_sem, cr_sem, xr_sem, gr_sem, th_sem, tr_sem, wr_sem, pr_sem, pq_sem, chain_sem,
):
    atom, wave = lax.axis_index("atom"), lax.axis_index("wave")
    here_y, here_x = lax.div(wave, 4), lax.rem(wave, 4)
    z, core = lax.div(atom, 2), lax.rem(atom, 2)
    partner = 2 * z + 1 - core
    ahead = 1 + 2 * core
    back = 3 - 2 * core

    def at(dy, dx):
        return lax.rem(here_y + dy, 4) * 4 + lax.rem(here_x + dx, 4)

    def opposite(dy, dx):
        return at(4 - dy, 4 - dx)

    PLACE_Y = (3, 1, 1, 3, 0, ahead, 0, back, 2, 1, 2, 3, 0, 2, 2)
    PLACE_X = (1, 1, 3, 3, ahead, 0, back, 0, 1, 2, 3, 2, 2, 0, 2)
    STEP_Y = (3, 0, 1, 0, 0, ahead, ahead)
    STEP_X = (0, 1, 0, 3, ahead, 0, ahead)
    corner = 1 + 2 * core

    def z_atom(dz, side):
        return 2 * lax.rem(z + dz, 8) + side

    def push(src, dst, ssem, rsem, axis, peer):
        return pltpu.make_async_remote_copy(
            src_ref=src, dst_ref=dst, send_sem=ssem, recv_sem=rsem,
            device_id={axis: peer}, device_id_type=pl.DeviceIdType.MESH,
        )

    def times(count, body, start=0):
        def step(k, carry):
            body(k)
            return carry

        lax.fori_loop(start, count, step, 0)

    barrier = pltpu.get_barrier_semaphore()

    def greet(axis, peer):
        pl.semaphore_signal(barrier, inc=1, device_id={axis: peer}, device_id_type=pl.DeviceIdType.MESH)

    for k in range(8):
        greet("wave", at(PLACE_Y[k], PLACE_X[k]))
    for d in (1, 7):
        greet("atom", z_atom(d, core))
    greet("atom", partner)

    def pass_on(k, d):
        peer = {"atom": z_atom(d, core)}
        pl.semaphore_signal(chain_sem.at[k], inc=1, device_id=peer, device_id_type=pl.DeviceIdType.MESH)

    loads = [
        pltpu.make_async_copy(src, dst, in_sem.at[k])
        for k, (src, dst) in enumerate(
            (
                (feat_in, feat), (species_in, species), (coords_in, coords), (embed_in, embed), (wc_in, w_charge_t),
                (widx_in, widx), (green_in, green), (wf_in, w_feat), (wp_in, w_pot), (wo_in, w_out),
            )
        )
    ]
    for load in loads:
        load.start()
    for load in loads[:5]:
        load.wait()

    hidden = feat[...].astype(F32)
    scale = lax.rsqrt(jnp.mean(hidden * hidden, axis=1, keepdims=True) + EPS)
    kinds = lax.broadcasted_iota(jnp.int32, (16, ATOMS), 0)
    onehot = (kinds == species[...]).astype(F32).astype(BF16)
    mixed_b = (hidden * scale + dot(onehot, embed[...], TN)).astype(BF16)
    mixed[...] = mixed_b
    cbuf[wave] = dot(w_charge_t[...], mixed_b, NT).astype(BF16)
    xbuf[wave] = coords[...]

    tmain[...] = jnp.zeros_like(tmain)
    tedge[...] = jnp.zeros_like(tedge)

    odd_wave = lax.rem(wave, 2)
    wave_sign = (1 - 2 * odd_wave).astype(F32)

    def prepare(slot, tabs, czs):
        place = xbuf[slot]
        j = lax.broadcasted_iota(jnp.int32, (HALF, ATOMS), 0).astype(F32) + 1.0
        tabs[0], tabs[1] = circle((2.0 * j - 0.5) * place[0:1])
        c, s = circle(j * place[1:2])
        c8, s8 = c[7:8], s[7:8]
        tabs[2], tabs[3] = c, c8 * c - s8 * s
        tabs[4], tabs[5] = s, s8 * c + c8 * s
        few = jnp.where(j == 1.0, 0.5 * place[0:1], (wave + 1).astype(F32) * place[2:3])
        tabs[6], tabs[7] = circle(few)
        hc, hs, zcw, zsw = tabs[6, 0:1, :], tabs[7, 0:1, :], tabs[6, 1:2, :], tabs[7, 1:2, :]
        rows = (hc * zcw, hc * zsw, hs * zcw, hs * zsw)
        zbuf[slot] = jnp.concatenate([*rows, jnp.zeros((4, ATOMS), F32)], axis=0)
        wide = cbuf[slot].astype(F32)
        for k in range(2):
            both = jnp.concatenate([rows[2 * k] * wide, rows[2 * k + 1] * wide], axis=0)
            czs[:, 128 * k : 128 * k + 128] = both.T.astype(BF16)

    def multiply(slot, tabs, czs):
        xc, xs = tabs[0], tabs[1]
        yc = jnp.concatenate([tabs[2], tabs[3]], axis=0)
        ys = jnp.concatenate([tabs[4], tabs[5]], axis=0)
        hc, hs = tabs[6, 0:1, :], tabs[7, 0:1, :]
        middle = lax.div(wave, 2)
        xcm, xsm = tabs[0, pl.ds(middle, 1), :], tabs[1, pl.ds(middle, 1), :]
        xcw = xcm * hc + wave_sign * (xsm * hs)
        xsw = xsm * hc - wave_sign * (xcm * hs)
        upper, lower = lax.div(wave, 8), lax.rem(wave, 8)
        ycw, ysw = tabs[2 + upper, pl.ds(lower, 1), :], tabs[4 + upper, pl.ds(lower, 1), :]
        for i in range(HALF):
            a, b = xc[i : i + 1], xs[i : i + 1]
            for k, part in enumerate((a * yc, a * ys, b * yc, b * ys)):
                ebuf[slot, 64 * i + N * k : 64 * i + N * (k + 1), :] = part.astype(BF16)
        r = lax.broadcasted_iota(jnp.int32, (N, ATOMS), 0)
        halves = jnp.where(r == 0, hc, jnp.where(r == 1, hs, 0.0))
        rest = jnp.zeros((N, ATOMS), F32)
        for k, row in enumerate((xcw, xsw, ycw, ysw)):
            rest = jnp.where(r == k + 1, row, rest)
        edge = (
            jnp.concatenate([xc, xs], axis=0), hc * yc, hc * ys, hs * yc, hs * ys, halves,
            xcw * yc, xsw * ys, xsw * yc, xcw * ys, rest,
        )
        for k, part in enumerate(edge):
            ebuf[slot, MAIN + N * k : MAIN + N * (k + 1), :] = part.astype(BF16)
        tmain[...] += dot(ebuf[slot, :LOW, :], czs[...])
        tedge[...] += dot(ebuf[slot, LOW:, :], cbuf[slot], NT)

    pl.semaphore_wait(barrier, 8 + 2 + 1)

    def c_copy(slot, peer):
        return push(cbuf.at[slot], cbuf.at[slot], send_sem.at[0], cr_sem.at[slot], "wave", peer)

    def x_copy(slot, peer):
        return push(xbuf.at[slot], xbuf.at[slot], send_sem.at[1], xr_sem.at[slot], "wave", peer)

    def send_on(slot, peer):
        x_copy(slot, peer).start()
        c_copy(slot, peer).start()

    for k in (1, 3, 0, 2, 4, 5, 6, 7):
        send_on(wave, at(PLACE_Y[k], PLACE_X[k]))

    for load in loads[5:]:
        load.wait()
    grid = green_rows(widx[0:1], widx[1:2], widx[2:3], green[...], atom)
    for k in range(N):
        gsend[k] = grid[8 * k : 8 * k + 8]
    gbuf[0] = gsend[wave]

    pass_on(0, 1)
    pass_on(1, 7)
    prepare(wave, tabs, czs)

    received = []
    for k in (1, 3, 0, 2, 4, 5, 6, 7, 9, 11, 8, 10, 12, 13, 14):
        code = PLACE_Y[k] + 4 * PLACE_X[k]
        if k < 6:
            code = code + 16 * STEP_Y[k] + 64 * STEP_X[k] + 256
        received.append(code)

    def receive(turn):
        code = pick(turn, received)
        slot = opposite(lax.rem(code, 4), lax.rem(lax.div(code, 4), 4))
        x_copy(slot, slot).wait_recv()
        c_copy(slot, slot).wait_recv()

        @pl.when(turn < 6)
        def _():
            send_on(slot, at(lax.rem(lax.div(code, 16), 4), lax.rem(lax.div(code, 64), 4)))

        @pl.when(turn == core)
        def _():
            send_on(slot, at(ahead, ahead))

        return slot

    def one(j, current):
        following = receive(j)
        for k in range(8):
            tabs_too[k] = tabs[k]
        multiply(current, tabs_too, czs)
        prepare(following, tabs, czs)
        return following

    current = lax.fori_loop(0, 8, one, wave)
    for k in (0, 1):
        pl.semaphore_wait(chain_sem.at[k], 1)
    pass_on(2, 1)
    pass_on(3, 7)
    current = lax.fori_loop(8, 15, one, current)
    for k in (2, 3):
        pl.semaphore_wait(chain_sem.at[k], 1)
    pass_on(4, 1)
    multiply(current, tabs, czs)

    low, high = slice(0, 128), slice(128, 256)
    xc, xs = slice(MAIN, MAIN + HALF), slice(MAIN + HALF, MAIN + N)
    for odd, sign in ((0, 1.0), (1, -1.0)):
        wedge[pl.ds(odd, HALF, stride=2), :] = tmain[xc, low] + sign * tmain[xs, high]
        wedge[pl.ds(N + odd, HALF, stride=2), :] = tmain[xs, low] - sign * tmain[xc, high]
    wedge[2 * N : 4 * N, :] = tmain[MAIN + N : MAIN + 3 * N, low] + tmain[MAIN + 3 * N : MAIN + 5 * N, high]
    wedge[4 * N :, :] = jnp.concatenate([tedge[...], jnp.zeros((5 * N, Q), F32)], axis=1)
    flat = tmain[MAIN + 5 * N : MAIN + 5 * N + 1, low] + tmain[MAIN + 5 * N + 1 : MAIN + 5 * N + 2, high]
    wedge[8 * N : 8 * N + 1, :] = flat

    def shard(ring, side):
        sign = (1 - 2 * side).astype(F32)
        c = pl.ds(pl.multiple_of(64 * ring, 64), 32)
        s = pl.ds(pl.multiple_of(64 * ring + 32, 32), 32)
        cosines = tmain[c, low] + sign * tmain[s, high]
        sines = tmain[s, low] - sign * tmain[c, high]
        edge = wedge[pl.ds(2 * ring + side, 8, stride=N), :]
        return jnp.concatenate([cosines, sines, edge, wedge[8 * N : 8 * N + 8, :]], axis=0)

    for k in range(8):
        thalf[k] = shard(jnp.int32(k), 1 - core).astype(BF16)
    half_copy = push(thalf, tother, th_sem.at[0], th_sem.at[1], "atom", partner)
    half_copy.start()

    @functools.partial(times, N, start=1)
    def _(d):
        peer = at(lax.div(d, 4), lax.rem(d, 4))
        push(gsend.at[peer], gbuf.at[d], send_sem.at[2], gr_sem.at[0], "wave", peer).start()

    half_copy.wait_recv()
    pl.semaphore_wait(chain_sem.at[4], 1)

    def t_copy(d):
        return push(tsend.at[d], trecv.at[d], send_sem.at[3], tr_sem.at[0], "atom", z_atom(d, core))

    for d in (4, 3, 5, 2, 6, 1, 7):
        owner = lax.rem(z + d, 8)
        tsend[d] = (shard(owner, core) + tother[owner].astype(F32)).astype(BF16)
        t_copy(d).start()
    total = shard(z, core) + tother[z].astype(F32)
    pre[...] = dot(mixed[...], w_feat[...])
    push(gsend.at[0:15], gbuf.at[1:16], send_sem.at[2], gr_sem.at[0], "wave", wave).wait_recv()
    gsum = gbuf[0]
    for k in range(1, N):
        gsum = gsum + gbuf[k]
    columns = jnp.concatenate([gsum, jnp.zeros((120, 128), F32)], axis=0).T


    all_shards = push(tsend.at[1:8], trecv.at[1:8], send_sem.at[3], tr_sem.at[0], "atom", atom)
    all_shards.wait_recv()
    for d in range(1, 8):
        total = total + trecv[d].astype(F32)
    wall[atom] = apply_green(total, columns).astype(BF16)

    def w_copy(slot, peer):
        return push(wall.at[slot], wall.at[slot], send_sem.at[4], wr_sem.at[slot], "atom", peer)

    w_copy(atom, partner).start()
    for d in (4, 3, 5, 2, 6, 1, 7):
        w_copy(atom, z_atom(d, core)).start()
    wmain[MAIN:, :] = jnp.zeros((128, 256), F32)

    def place_pair(d):
        ring = lax.rem(z + 8 - d, 8)
        w_copy(2 * ring + 1 - core, partner).wait_recv()
        first, second = wall[2 * ring].astype(F32), wall[2 * ring + 1].astype(F32)
        rows = pl.ds(pl.multiple_of(64 * ring, 64), 64)
        wmain[rows, low] = second[0:64] + first[0:64]
        wmain[rows, high] = jnp.concatenate([second[32:64] - first[32:64], first[0:32] - second[0:32]], axis=0)
        wedge[pl.ds(2 * ring, 8, stride=N), :] = first[64:72]
        wedge[pl.ds(2 * ring + 1, 8, stride=N), :] = second[64:72]

    order = (0, 1, 7, 2, 6, 3, 5, 4)
    for j, d in enumerate(order):
        if d:
            source = z_atom(8 - d, core)
            w_copy(source, partner).wait_recv()
            w_copy(source, partner).start()
        if j >= 4:
            place_pair(order[j - 4])
    for d in order[-4:]:
        place_pair(d)
    tail = wall[0, 72:80, :].astype(F32)
    fc, sc, fs, ss = (wedge[pl.ds(k, HALF, stride=2), :] for k in (0, 1, N, N + 1))
    wmain[xc, low], wmain[xc, high] = sc + fc, ss - fs
    wmain[xs, low], wmain[xs, high] = ss + fs, fc - sc
    wmain[MAIN + N : MAIN + 3 * N, low] = wedge[2 * N : 4 * N, :]
    wmain[MAIN + 3 * N : MAIN + 5 * N, high] = wedge[2 * N : 4 * N, :]
    wmain[MAIN + 5 * N : MAIN + 5 * N + 1, low] = tail[0:1]
    wmain[MAIN + 5 * N + 1 : MAIN + 5 * N + 2, high] = tail[0:1]
    for k in range(5):
        for half in (low, high):
            wt[half, 128 * k : 128 * k + 128] = wmain[128 * k : 128 * k + 128, half].T.astype(BF16)
    edges = jnp.concatenate([wedge[4 * N : 8 * N, :], tail, jnp.zeros((56, 128), F32)], axis=0).T
    column = lax.broadcasted_iota(jnp.int32, (Q, 128), 1)
    wflat[...] = jnp.where(column == 4 * N, 0.0, edges[:Q]).astype(BF16)

    prelay[7] = jnp.zeros((Q, ATOMS), BF16)

    def partial(slot):
        u = dot(wt[:, :LOW], ebuf[slot, :LOW, :])
        v = zbuf[slot]
        out = dot(wflat[:, : 5 * N], ebuf[slot, LOW:, :])
        for k in range(4):
            out = out + v[k : k + 1] * u[Q * k : Q * k + Q]
        return out

    def up_copy(k, peer):
        return push(psend.at[k], precv.at[k], send_sem.at[5], pr_sem.at[k], "wave", peer)

    def relay_copy(k, r, peer):
        return push(psend.at[k], prelay.at[r], send_sem.at[5], pq_sem.at[r], "wave", peer)

    across = 4 - corner
    turns = (14, 8 + corner, 8, 10, 8 + across, 12, 13, 6, 7, 0, 2, corner, across, 4, 5)

    @functools.partial(times, 15)
    def _(j):
        k = pick(j, turns)
        slot = opposite(pick(k, PLACE_Y), pick(k, PLACE_X))
        value = partial(slot)

        @pl.when(k < 6)
        def _():
            relay_copy(0, k, slot).wait_recv()

        @pl.when(k == corner)
        def _():
            relay_copy(0, 6, slot).wait_recv()

        value = value + prelay[jnp.where(k < 6, k, 7)].astype(F32)
        value = value + prelay[jnp.where(k == corner, 6, 7)].astype(F32)
        psend[k] = value.astype(BF16)

        @pl.when(k < 8)
        def _():
            up_copy(k, slot).start()

        @pl.when(k >= 8)
        def _():
            step = k - 8
            relay_copy(k, step, opposite(pick(step, STEP_Y), pick(step, STEP_X))).start()

    potential = partial(wave)
    for k in (6, 7, 0, 2, 1, 3, 4, 5):
        up_copy(k, wave).wait_recv()
        potential = potential + precv[k].astype(F32)
    potential_b = potential.T.astype(BF16)
    before = pre[...] + dot(potential_b, w_pot[...])
    activation = (before / (1.0 + jnp.exp(-before))).astype(BF16)
    out[...] = (feat[...].astype(F32) + dot(activation, w_out[...])).astype(BF16)

    half_copy.wait_send()
    all_shards.wait_send()
    push(cbuf.at[0:15], cbuf.at[0:15], send_sem.at[0], cr_sem.at[0], "wave", wave).wait_send()
    push(xbuf.at[0:15], xbuf.at[0:15], send_sem.at[1], xr_sem.at[0], "wave", wave).wait_send()
    push(gsend.at[0:15], gbuf.at[1:16], send_sem.at[2], gr_sem.at[0], "wave", wave).wait_send()
    push(wall.at[0:15], wall.at[0:15], send_sem.at[4], wr_sem.at[0], "atom", atom).wait_send()
    push(psend, psend, send_sem.at[5], pr_sem.at[0], "wave", wave).wait_send()


def shards(features, species, coords, wave_index, green, embed, w_charge, w_feat, w_pot, w_out):
    operands = (
        features, species.reshape(1, -1), coords, wave_index, green.reshape(1, -1),
        embed, w_charge.T, w_feat, w_pot, w_out,
    )
    return pl.pallas_call(
        kernel,
        out_shape=pltpu.VMEM(features.shape, BF16),
        in_specs=[pl.BlockSpec(memory_space=pl.ANY)] * 10,
        out_specs=pl.BlockSpec(memory_space=pltpu.VMEM),
        scratch_shapes=[pltpu.VMEM(v.shape, v.dtype) for v in operands]
        + [
            pltpu.VMEM((N, Q, ATOMS), BF16),
            pltpu.VMEM((N, 3, ATOMS), F32),
            pltpu.VMEM((N, 8, 128), F32),
            pltpu.VMEM((N, 8, 128), F32),
            pltpu.VMEM((N, ROWS, ATOMS), BF16),
            pltpu.VMEM((N, 8, ATOMS), F32),
            pltpu.VMEM((8, HALF, ATOMS), F32),
            pltpu.VMEM((8, HALF, ATOMS), F32),
            pltpu.VMEM((ATOMS, 256), BF16),
            pltpu.VMEM((LOW, 256), F32),
            pltpu.VMEM((5 * N, Q), F32),
            pltpu.VMEM((9 * N, 128), F32),
            pltpu.VMEM((8, SHARD, 128), BF16),
            pltpu.VMEM((8, SHARD, 128), BF16),
            pltpu.VMEM((8, SHARD, 128), BF16),
            pltpu.VMEM((8, SHARD, 128), BF16),
            pltpu.VMEM((N, SHARD, 128), BF16),
            pltpu.VMEM((MAIN + 128, 256), F32),
            pltpu.VMEM((256, MAIN + 128), BF16),
            pltpu.VMEM((Q, 128), BF16),
            pltpu.VMEM((15, Q, ATOMS), BF16),
            pltpu.VMEM((8, Q, ATOMS), BF16),
            pltpu.VMEM((8, Q, ATOMS), BF16),
            pltpu.VMEM((ATOMS, 128), BF16),
            pltpu.VMEM((ATOMS, 256), F32),
        ]
        + [pltpu.SemaphoreType.DMA((n,)) for n in (10, 6, N, N, 1, 2, 1, N, 8, 7)]
        + [pltpu.SemaphoreType.REGULAR((5,))],
        compiler_params=pltpu.CompilerParams(
            collective_id=0, has_side_effects=True, vmem_limit_bytes=60 * 1024 * 1024
        ),
        name="ewald",
    )(*operands)


def solution(mesh):
    placed = (
        P(("atom", "wave"), None),
        P(("atom", "wave")),
        P(None, ("atom", "wave")),
        P(None, "wave"),
        P("wave"),
        P(),
        P(),
        P(),
        P(),
        P(),
    )
    return jax.shard_map(
        shards, mesh=mesh, in_specs=placed, out_specs=P(("atom", "wave"), None), check_vma=False
    )
```
